32 devices in a mesh: gx: 8 (over y, x, core), gy: 4 (over z).
Axes of the slice: x: 2, y: 2, z: 4, core: 2. Of those that a mesh axis runs over, the one named last changes fastest.
Arguments:
- volts: float32 [32, 4, 64, 512], P(None, None, 'gx', 'gy'), may hold values from -6 to 6
- cap: float32 [4, 64, 512], P(None, 'gx', 'gy'), may hold values from 0.05 to 1
- cond_x: float32 [4, 64, 512], P(None, 'gx', 'gy'), may hold values from 0.5 to 2
- cond_y: float32 [4, 64, 512], P(None, 'gx', 'gy'), may hold values from 0.5 to 2
- via: float32 [4, 64, 512], P(None, 'gx', 'gy'), may hold values from 0.2 to 2
- waveforms: float32 [64, 64], replicated, may hold values from -6 to 6
- placement: int32 [262144, 1], P(('gx', 'gy')), may hold values from 0 to 31; in each aligned block of 8192 rows (0 to 8191, 8192 to 16383, ...) at most 512 rows name the same one
- cells: int32 [262144], P(('gx', 'gy')), may hold values from 0 to 1023
- wave_ids: int32 [262144], P(('gx', 'gy')), may hold values from 0 to 63
- amps: float32 [262144], P(('gx', 'gy')), may hold values from 0.5 to 4
Outputs:
- volts_out: float32 [32, 4, 64, 512], P(None, None, 'gx', 'gy')
- residual: float32 [32, 4, 64, 512], P(None, None, 'gx', 'gy')
The draws below stay inside these ranges and needn't reach their ends.
Inputs may be any that keep to these rules, and one draw needn't show every extreme that they name: `placement`: in each device's block of 8192 rows no tile is named more than 512 times, a bound that some block reaches.
All inputs are finite; a program needn't handle non-finite values.
Results may differ from the reference program's by a relative error of at most 0.0029.
Values may be sent and summed in bfloat16 or wider, within the bound.
A program may use at most 64 MiB of HBM per device.

```python
import math
import jax
import jax.numpy as jnp
import numpy as np
from jax import lax

SCEN = 32
LAYERS = 4
WAVES = 64
CX = 8
CY = 128
INST_DEV = 8192
STEPS = 2
ITERS = 3
CAP = 512
INSTANCES = 262144
NX = 64
NY = 512
N_GY = 4
DEVICES = 32


def touch_ends(drawn, key, least, largest):
    place = [jax.random.randint(jax.random.fold_in(key, axis), (), 0, length) for axis, length in enumerate(drawn.shape)]
    widest = drawn.shape.index(max(drawn.shape))
    beside = place[:widest] + [(place[widest] + 1) % drawn.shape[widest]] + place[widest + 1:]
    return drawn.at[tuple(place)].set(least).at[tuple(beside)].set(largest)


def steps_of(rng, dims, shards, smallest, high):
    def one(axis_at, parts):
        draws = jax.random.uniform(jax.random.fold_in(jax.random.fold_in(rng, 6), axis_at), (parts,), jnp.float32, smallest / len(shards), high / len(shards))
        return jnp.repeat(jnp.exp(draws), dims[axis_at] // parts).reshape((-1,) + (1,) * (len(dims) - axis_at - 1))

    factor_of = one(*shards[0])
    for cut in shards[1:]:
        factor_of = factor_of * one(*cut)
    return factor_of


def assign_block(rng, own, number, rows, number_of, top, limit, slope):
    order = jax.random.permutation(rng, number_of)
    heavy_load, usual = shares(number_of, rows * top, limit, slope, True), shares(number_of, rows * top, limit, slope, False)
    places = jnp.arange(number_of)

    def named(tallies, rotation):
        used = int((tallies > 0).sum())
        fixed = max(1, used // 4)
        passed = fixed + (places - fixed + rotation * (used - fixed)) % max(1, number_of - fixed)
        return jnp.zeros((number_of,), jnp.int32).at[order[jnp.where(places < fixed, places, passed)]].set(jnp.asarray(tallies, jnp.int32))

    tallies = jnp.where(number % 4 == 0, named(heavy_load, number // 4), named(usual, number - number // 4 - 1))
    mixed = jax.random.permutation(jax.random.fold_in(own, 3), number_of)
    donor, taker = mixed[0:number_of // 2 * 2:2], mixed[1:number_of // 2 * 2:2]
    slack = jnp.minimum(tallies[donor] - 1, limit - tallies[taker]) // 2
    slack = jnp.where((donor == order[0]) | (taker == order[0]) | (tallies[taker] == 0), 0, jnp.maximum(slack, 0))
    passed = jax.random.randint(jax.random.fold_in(own, 4), (number_of // 2,), 0, 1 << 20) % (slack + 1)
    tallies = tallies.at[donor].add(-passed).at[taker].add(passed)
    labels = jnp.searchsorted(jnp.cumsum(tallies), jnp.arange(rows * top), side="right").astype(jnp.int32)
    grid = labels.reshape(top, rows).T
    grid = grid[jax.random.permutation(jax.random.fold_in(own, 1), rows)]
    rotation = jax.random.randint(jax.random.fold_in(own, 2), (rows, 1), 0, top)
    return jnp.take_along_axis(grid, (jnp.arange(top)[None, :] + rotation) % top, axis=1)


def shares(number_of, total, limit, slope, full):
    loads = [(1 << 20) // math.isqrt(grade ** slope) + 1 for grade in range(1, number_of + 1)]
    largest = limit if full else min(limit, max(-(-total // number_of), total * loads[0] // sum(loads)))
    least = 1 if total - largest >= number_of - 1 else 0
    counts, rest = [largest] + [least] * (number_of - 1), total - largest - least * (number_of - 1)
    while rest > 0:
        free = [i for i in range(1, number_of) if counts[i] < largest] or [i for i in range(1, number_of) if counts[i] < limit]
        mass, left = sum([loads[i] for i in free]), rest
        for i in free:
            more = min(limit - counts[i], max(1, left * loads[i] // mass), rest)
            counts[i] = counts[i] + more
            rest = rest - more
    return np.array(counts)


def normal_values(stream_key, shape, spread, most, split=(), held_as=jnp.bfloat16):
    values = spread * jax.random.normal(stream_key, shape, jnp.float32)
    if split:
        values = values * steps_of(stream_key, shape, split, -0.22, 0.18)
    return jnp.clip(values, -most, most).astype(held_as)


def setup_inputs(seed: int = 0) -> dict:
    arg_keys = jax.random.split(jax.random.key(seed), 11)
    volts = normal_values(arg_keys[0], (SCEN, LAYERS, NX, NY), 1.0, 6.0, ((2, 8), (3, 4)), jnp.float32)
    cap = jnp.clip(jnp.exp(math.log(1.0) - 2.9957323 * jax.random.uniform(arg_keys[1], (LAYERS, NX, NY), jnp.float32) ** steps_of(arg_keys[1], (LAYERS, NX, NY), ((1, 8), (2, 4)), -0.2, 0.2)), 0.05, 1.0)
    cond_x = jnp.clip(jnp.exp(math.log(2.0) - 1.3862944 * jax.random.uniform(arg_keys[2], (LAYERS, NX, NY), jnp.float32) ** steps_of(arg_keys[2], (LAYERS, NX, NY), ((1, 8), (2, 4)), -0.2, 0.2)), 0.5, 2.0)
    cond_y = jnp.clip(jnp.exp(math.log(2.0) - 1.3862944 * jax.random.uniform(arg_keys[3], (LAYERS, NX, NY), jnp.float32) ** steps_of(arg_keys[3], (LAYERS, NX, NY), ((1, 8), (2, 4)), -0.2, 0.2)), 0.5, 2.0)
    via = jnp.clip(jnp.exp(math.log(2.0) - 2.3025851 * jax.random.uniform(arg_keys[4], (LAYERS, NX, NY), jnp.float32) ** steps_of(arg_keys[4], (LAYERS, NX, NY), ((1, 8), (2, 4)), -0.2, 0.2)), 0.2, 2.0)
    waveforms = normal_values(arg_keys[5], (STEPS * SCEN, WAVES), 1.0, 6.0, (), jnp.float32)
    placement_keys = jax.random.split(jax.random.fold_in(arg_keys[6], 1), INSTANCES // INST_DEV)
    placement_turns = jax.random.permutation(jax.random.fold_in(arg_keys[6], 3), INSTANCES // INST_DEV)
    placement = jax.vmap(lambda own, number: assign_block(jax.random.fold_in(arg_keys[6], 2), own, number, INST_DEV, DEVICES, 1, CAP, 2))(placement_keys, placement_turns).reshape((INSTANCES, 1))
    cells = touch_ends(jax.random.randint(arg_keys[7], (INSTANCES,), 0, CX * CY), jax.random.fold_in(arg_keys[7], 1), 0, (CX * CY) - 1).astype(jnp.int32)
    wave_ids = touch_ends(jax.random.randint(arg_keys[8], (INSTANCES,), 0, WAVES), jax.random.fold_in(arg_keys[8], 1), 0, WAVES - 1).astype(jnp.int32)
    amps = jnp.clip(jnp.exp(math.log(4.0) - 2.0794415 * jax.random.uniform(arg_keys[9], (INSTANCES,), jnp.float32) ** steps_of(arg_keys[9], (INSTANCES,), ((0, 32),), -0.2, 0.2)), 0.5, 4.0)
    return dict(volts=volts, cap=cap, cond_x=cond_x, cond_y=cond_y, via=via, waveforms=waveforms, placement=placement, cells=cells, wave_ids=wave_ids, amps=amps)


def operate(field, cap, cond_x, cond_y, via):
    cond_x_low = jnp.pad(cond_x, ((0, 0), (1, 0), (0, 0)))[:, :-1, :]
    cond_y_low = jnp.pad(cond_y, ((0, 0), (0, 0), (1, 0)))[:, :, :-1]
    via_low = jnp.pad(via, ((1, 0), (0, 0), (0, 0)))[:-1]
    padded = jnp.pad(field, ((0, 0), (0, 0), (1, 1), (1, 1)))
    upper = jnp.pad(field, ((0, 0), (0, 1), (0, 0), (0, 0)))[:, 1:]
    lower = jnp.pad(field, ((0, 0), (1, 0), (0, 0), (0, 0)))[:, :-1]
    result = cap * field
    result = result + cond_x * (field - padded[:, :, 2:, 1:-1])
    result = result + cond_x_low * (field - padded[:, :, :-2, 1:-1])
    result = result + cond_y * (field - padded[:, :, 1:-1, 2:])
    result = result + cond_y_low * (field - padded[:, :, 1:-1, :-2])
    result = result + via * (field - upper) + via_low * (field - lower)
    return result

def gram(left, right):
    left_rows = left.reshape(left.shape[0], -1)
    right_rows = right.reshape(right.shape[0], -1)
    return lax.dot_general(left_rows, right_rows, (((1,), (1,)), ((), ())), precision=lax.Precision.HIGHEST)

def combine(coef, field):
    return jnp.einsum('st,slxy->tlxy', coef, field, precision=lax.Precision.HIGHEST)

def spd_solve(matrix, right):
    factor = jnp.linalg.cholesky(matrix)
    return jax.scipy.linalg.cho_solve((factor, True), right)

def reference(volts, cap, cond_x, cond_y, via, waveforms, placement, cells, wave_ids, amps):
    tile = placement[:, 0]
    row_x = tile // N_GY * CX + cells // CY
    col_y = tile % N_GY * CY + cells % CY
    flat = (row_x * NY + col_y).astype(jnp.int32)
    currents = (waveforms[:, wave_ids] * amps[None, :]).astype(jnp.bfloat16)
    injected = jax.ops.segment_sum(currents.astype(jnp.float32).T, flat, num_segments=NX * NY)
    injected = injected.T.reshape(STEPS, SCEN, NX, NY)
    voltage = volts
    residual = volts
    for step in range(STEPS):
        rhs = cap * voltage
        rhs = rhs.at[:, 0].add(-injected[step])
        iterate = voltage
        residual = rhs - operate(iterate, cap, cond_x, cond_y, via)
        direction = residual
        norm_gram = gram(residual, residual)
        for sweep in range(ITERS):
            image = operate(direction, cap, cond_x, cond_y, via)
            curve_gram = gram(direction, image)
            step_coef = spd_solve(curve_gram, norm_gram)
            iterate = iterate + combine(step_coef, direction)
            residual = residual - combine(step_coef, image)
            if sweep + 1 < ITERS:
                new_gram = gram(residual, residual)
                turn_coef = spd_solve(norm_gram, new_gram)
                direction = residual + combine(turn_coef, direction)
                norm_gram = new_gram
        voltage = iterate
    return (voltage, residual)
```

```python
import functools

import jax
import jax.numpy as jnp
from jax import lax
from jax.experimental import pallas as pl
from jax.experimental.pallas import tpu as pltpu
from jax.sharding import PartitionSpec as P

ITERS = 3
SUBLANES = 8
SCALE = 6.0
SHIFT = 1.125
LANES = 128
MESH = pl.DeviceIdType.MESH
NT = (((1,), (1,)), ((), ()))
F32 = jnp.float32
BF16 = jnp.bfloat16


def split3(x):
    first = x.astype(BF16).astype(F32)
    rest = x - first
    second = rest.astype(BF16).astype(F32)
    return first, second, rest - second


def rows_iota(rows, cols):
    return lax.broadcasted_iota(jnp.int32, (rows, cols), 0)


def bin_kernel(devices, capacity, target_ref, cell_ref, wave_ref, amp_ref, out_ref, acc_ref):
    blocks, width = target_ref.shape
    rows = out_ref.shape[1]
    before = (
        rows_iota(width, width) < lax.broadcasted_iota(jnp.int32, (width, width), 1)
    ).astype(F32).astype(BF16)
    acc_ref[...] = jnp.zeros_like(acc_ref)

    def step(b, base):
        target = target_ref[pl.ds(b, 1), :]
        hits = (rows_iota(devices, width) == target).astype(F32)
        ahead = jnp.dot(hits.astype(BF16), before, preferred_element_type=F32)
        position = jnp.sum(hits * (ahead + base), axis=0, keepdims=True)
        slot = target * capacity + position.astype(jnp.int32)
        row_hits = rows_iota(rows, width) == (slot >> 7)
        lane_hits = (rows_iota(LANES, width) == (slot & 127)).astype(F32).astype(BF16)
        code = cell_ref[pl.ds(b, 1), :] * 64 + wave_ref[pl.ds(b, 1), :]
        parts = split3(amp_ref[pl.ds(b, 1), :]) + (
            (code >> 8).astype(F32),
            (code & 255).astype(F32),
        )
        for i, part in enumerate(parts):
            left = jnp.where(row_hits, part, 0.0).astype(BF16)
            acc_ref[i] += lax.dot_general(left, lane_hits, NT, preferred_element_type=F32)
        return base + jnp.sum(hits, axis=1, keepdims=True)

    lax.fori_loop(0, blocks, step, jnp.zeros((devices, 1), F32), unroll=2)
    out_ref[0] = (acc_ref[2] + acc_ref[1]) + acc_ref[0]
    out_ref[1] = acc_ref[3] * 256.0 + acc_ref[4]


def bin_instances(devices, capacity, target, cells, wave_ids, amps):
    width = 512
    shape = (target.shape[0] // width, width)
    rows = devices * capacity // LANES
    return pl.pallas_call(
        functools.partial(bin_kernel, devices, capacity),
        out_shape=jax.ShapeDtypeStruct((2, rows, LANES), F32),
        in_specs=[pl.BlockSpec(memory_space=pltpu.VMEM)] * 4,
        out_specs=pl.BlockSpec(memory_space=pltpu.VMEM),
        scratch_shapes=[pltpu.VMEM((5, rows, LANES), F32)],
        name="bin",
    )(*[x.reshape(shape) for x in (target, cells, wave_ids, amps)])


def inject_kernel(parts, arrived_ref, wave_ref, out_ref, acc_ref):
    sources, width = arrived_ref.shape[1:]
    kinds = wave_ref.shape[1]
    outs = wave_ref.shape[0]
    low_count = out_ref.shape[1] // parts
    table = jnp.concatenate(split3(wave_ref[...]), axis=0).astype(BF16)
    acc_ref[...] = jnp.zeros_like(acc_ref)

    def step(i, carry):
        amp = arrived_ref[0, pl.ds(i, 1), :]
        code = arrived_ref[1, pl.ds(i, 1), :].astype(jnp.int32)
        cell = code >> 6
        low, high = cell % low_count, cell // low_count
        kind_hits = (rows_iota(kinds, width) == (code & 63)).astype(F32).astype(BF16)
        picked = jnp.dot(table, kind_hits, preferred_element_type=F32)
        wave = (picked[2 * outs :] + picked[outs : 2 * outs]) + picked[:outs]
        currents = (wave * amp).astype(BF16).astype(F32)
        low_hits = (rows_iota(low_count, width) == low).astype(F32).astype(BF16)
        left = jnp.concatenate(
            [jnp.where(high == h, currents, 0.0).astype(BF16) for h in range(parts)], axis=0
        )
        acc_ref[...] += lax.dot_general(left, low_hits, NT, preferred_element_type=F32)
        return carry

    lax.fori_loop(0, sources, step, 0, unroll=2)
    for h in range(parts):
        out_ref[:, h * low_count : (h + 1) * low_count] = acc_ref[h * outs : (h + 1) * outs]


def inject(arrived, waveforms, die_cells):
    parts = 4
    return pl.pallas_call(
        functools.partial(inject_kernel, parts),
        out_shape=jax.ShapeDtypeStruct((waveforms.shape[0], die_cells), F32),
        in_specs=[pl.BlockSpec(memory_space=pltpu.VMEM)] * 2,
        out_specs=pl.BlockSpec(memory_space=pltpu.VMEM),
        scratch_shapes=[pltpu.VMEM((parts * waveforms.shape[0], die_cells // parts), F32)],
        name="inject",
    )(arrived, waveforms)


def across(tile, k):
    return jnp.broadcast_to(tile[:, k : k + 1], tile.shape)


def down(tile, a):
    return jnp.broadcast_to(tile[a : a + 1, :], tile.shape)


def eliminate_panel(tiles, p):
    tile, k = tiles[p], SUBLANES * p
    sub = rows_iota(SUBLANES, LANES)
    columns = [across(tile, k + b) for b in range(SUBLANES)]
    pivot = [[down(columns[b], a) for b in range(SUBLANES)] for a in range(SUBLANES)]
    right = [down(tile, a) for a in range(SUBLANES)]
    inverse = []
    for a in range(SUBLANES):
        inverse.append(1.0 / pivot[a][a])
        for b in range(a + 1, SUBLANES):
            factor = pivot[a][b] * inverse[a]
            right[b] = right[b] - factor * right[a]
            for c in range(b, SUBLANES):
                pivot[b][c] = pivot[b][c] - factor * pivot[a][c]
    solved = [None] * SUBLANES
    for a in reversed(range(SUBLANES)):
        row = right[a]
        for b in reversed(range(a + 1, SUBLANES)):
            row = row - pivot[a][b] * solved[b]
        solved[a] = row * inverse[a]
    fresh = []
    for i, other in enumerate(tiles):
        if i == p:
            result = solved[0]
            for a in range(1, SUBLANES):
                result = jnp.where(sub == a, solved[a], result)
        else:
            result = other
            for b in range(SUBLANES):
                result = result - across(other, k + b) * solved[b]
        fresh.append(result)
    return fresh


def halves(x):
    high = x.astype(BF16)
    return high, (x - high.astype(F32)).astype(BF16)


def grid_kernel(
    nx, ny, steps, layers, tile_x,
    v_in, inj, coef, v, r,
    k0, k1, k2, basis, xl, ys, yl, gl, hl,
    xsend, xrecv, ysend, yrecv, gsend, grecv, hsend, hrecv,
):
    gx, gy = lax.axis_index("gx"), lax.axis_index("gy")
    size = v.shape[2]
    count = layers * tile_x
    halos = 1 + ITERS * steps
    packed = LANES // size
    part = size // packed
    spans = ((0, 3 * part), (3 * part, 2 * part), (5 * part, part))
    lane = lax.broadcasted_iota(jnp.int32, (size, LANES), 1)
    group = lax.broadcasted_iota(jnp.int32, (part, LANES), 1) // size
    edges = [l * tile_x + x for l in range(layers) for x in (0, tile_x - 1)]
    inner = [c for c in range(count) if c not in edges]
    fields = (k0, k1, k2)

    def at(ref, c):
        return ref.at[c // tile_x, c % tile_x]

    def x_copies(src, e):
        return [
            pltpu.make_async_remote_copy(
                src.at[:, tile_x - 1 if side == 0 else 0], xl.at[e, side],
                xsend.at[e, side], xrecv.at[e, side],
                device_id={"gx": lax.rem(gx + (1 if side == 0 else nx - 1), nx)},
                device_id_type=MESH,
            )
            for side in range(2)
        ]

    def y_copies(e):
        return [
            pltpu.make_async_remote_copy(
                ys.at[e, side], yl.at[e, side], ysend.at[e, side], yrecv.at[e, side],
                device_id={"gy": lax.rem(gy + (1 if side == 0 else ny - 1), ny)},
                device_id_type=MESH,
            )
            for side in range(2)
        ]

    def start(copies, me, n):
        pl.when(me < n - 1)(copies[0].start)
        pl.when(me > 0)(copies[1].start)

    def finish(copies, me, n):
        @pl.when(me > 0)
        def _():
            copies[0].wait_recv()
            copies[1].wait_send()

        @pl.when(me < n - 1)
        def _():
            copies[1].wait_recv()
            copies[0].wait_send()

    def arrive(src, e):
        finish(x_copies(src, e), gx, nx)
        finish(y_copies(e), gy, ny)

    class Rim:
        def __init__(self):
            self.last = jnp.zeros((size, LANES), F32)
            self.first = self.last

        def add(self, c, f):
            self.last = jnp.where(lane == c, pltpu.roll(f, (c + 1) % LANES, 1), self.last)
            self.first = jnp.where(lane == c, pltpu.roll(f, c, 1) if c else f, self.first)

        def send(self, e):
            ys[e, 0] = self.last
            ys[e, 1] = self.first
            start(y_copies(e), gy, ny)

    def stencil(src, e, own, emit, after_edges):
        y_low, y_high = yl[e, 0], yl[e, 1]
        for n, c in enumerate(edges + inner):
            l, x = divmod(c, tile_x)
            f = src[l, x]

            def k(i):
                return coef[i, c : c + 1, :]

            high = src[l, x + 1] if x + 1 < tile_x else xl[e, 1, l]
            low = src[l, x - 1] if x else xl[e, 0, l]
            total = k(own) * f - k(2) * high - k(3) * low
            after = jnp.where(
                lane == LANES - 1, pltpu.roll(y_high, LANES - 1 - c, 1), pltpu.roll(f, LANES - 1, 1)
            )
            ahead = jnp.where(
                lane == 0, pltpu.roll(y_low, LANES - c, 1) if c else y_low, pltpu.roll(f, 1, 1)
            )
            total = total - k(4) * after - k(5) * ahead
            if l + 1 < layers:
                total = total - k(6) * src[l + 1, x]
            if l:
                total = total - k(7) * src[l - 1, x]
            emit(c, total)
            if n + 1 == len(edges):
                after_edges()

    def split(j, c, f):
        high, low = halves(f)
        cols = slice(c * LANES, (c + 1) * LANES)
        basis[j * size : (j + 1) * size, cols] = high
        basis[(ITERS + 1 + j) * size : (ITERS + 2 + j) * size, cols] = low

    def grams(left, j):
        def rows(i):
            return [basis[b * size : (b + 1) * size, :] for b in (i, ITERS + 1 + i)]

        every = [block for i in left for block in rows(i)]
        product = lax.dot_general(
            jnp.concatenate(every, axis=0), jnp.concatenate(rows(j), axis=0), NT,
            preferred_element_type=F32,
        )
        product = product[:, :size] + product[:, size:]
        return [
            product[2 * i * size : (2 * i + 1) * size] + product[(2 * i + 1) * size : (2 * i + 2) * size]
            for i in range(len(left))
        ]

    def pack(matrix):
        return jnp.concatenate([matrix[i * part : (i + 1) * part] for i in range(packed)], axis=1)

    def gather(land, step, g, ssem, rsem, axis, me, n):
        rows = pl.ds(spans[g][0], spans[g][1])
        return [
            pltpu.make_async_remote_copy(
                land.at[step, me, rows], land.at[step, me, rows],
                ssem.at[step, g, j], rsem.at[step, g, j],
                device_id={axis: lax.rem(me + j, n)}, device_id_type=MESH,
            )
            for j in range(1, n)
        ]

    def along_x(step, g):
        return gather(gl, step, g, gsend, grecv, "gx", gx, nx)

    def along_y(step, g):
        return gather(hl, step, g, hsend, hrecv, "gy", gy, ny)

    def add_start(step, g, matrices):
        for i, matrix in enumerate(matrices):
            gl[step, gx, pl.ds(spans[g][0] + i * part, part), :] = pack(matrix)
        for copy in along_x(step, g):
            copy.start()

    def landed(land, copies, step, g, n):
        for copy in copies:
            copy.wait()
        first, rows = spans[g]
        total = land[step, 0, first : first + rows, :]
        for j in range(1, n):
            total = total + land[step, j, first : first + rows, :]
        return total

    def add_turn(step, g):
        total = landed(gl, along_x(step, g), step, g, nx)
        hl[step, gy, pl.ds(*spans[g]), :] = total
        for copy in along_y(step, g):
            copy.start()

    def add_finish(step, g):
        total = landed(hl, along_y(step, g), step, g, ny)
        return [total[i * part : (i + 1) * part] for i in range(spans[g][1] // part)]

    def place(matrix, g, block):
        shift = ((block - g) * size) % LANES
        return pltpu.roll(matrix, shift, 1) if shift else matrix

    for e in range(halos):
        for me, n, land in ((gx, nx, xl), (gy, ny, yl)):
            for side, last in ((0, 0), (1, n - 1)):
                @pl.when(me == last)
                def _():
                    land[e, side] = jnp.zeros(land.shape[2:], F32)

    barrier = pltpu.get_barrier_semaphore()
    for axis, me, n in (("gx", gx, nx), ("gy", gy, ny)):
        for j in range(1, n):
            pl.semaphore_signal(
                barrier, inc=1, device_id={axis: lax.rem(me + j, n)}, device_id_type=MESH
            )
    pl.semaphore_wait(barrier, nx + ny - 2)

    rim = Rim()
    for c in range(count):
        f = v_in[pl.ds(c, size, stride=count), :]
        v[c // tile_x, c % tile_x] = f
        rim.add(c, f)
    start(x_copies(v, 0), gx, nx)
    rim.send(0)
    arrive(v, 0)
    rim = Rim()

    def first_residual(c, total):
        f = -SCALE * total
        if c < tile_x:
            f = f - inj[:size, c * LANES : (c + 1) * LANES]
        k0[c // tile_x, c % tile_x] = f
        r[c // tile_x, c % tile_x] = f
        rim.add(c, f)

    stencil(v, 0, 1, first_residual, lambda: start(x_copies(k0, 1), gx, nx))
    rim.send(1)

    def time_step(step, carry):
        e = 1 + ITERS * step
        for c in range(count):
            split(0, c, k0[c // tile_x, c % tile_x])
        moments = grams([0], 0)
        for j in range(1, ITERS + 1):
            arrive(fields[j - 1], e + j - 1)
            if j > 1:
                add_turn(step, j - 2)
            rim = Rim()

            def next_field(c, total):
                split(j, c, total)
                if j < ITERS:
                    fields[j][c // tile_x, c % tile_x] = total
                    rim.add(c, total)

            def send_edges():
                if j < ITERS:
                    start(x_copies(fields[j], e + j), gx, nx)

            stencil(fields[j - 1], e + j - 1, 0, next_field, send_edges)
            if j < ITERS:
                rim.send(e + j)
            moments = moments + grams([j - 1, j] if j < ITERS else [j - 1], j)
            add_start(step, j - 1, moments)
            moments = []
        m = add_finish(step, 0)
        add_turn(step, ITERS - 1)
        m = m + add_finish(step, 1)
        m.append(jnp.zeros_like(m[0]))
        shifted_m = [SCALE * (m[i + 1] + SHIFT * m[i]) for i in range(len(m) - 1)]
        tiles = []
        for i in range(ITERS):
            for g in range(packed):
                tile = place(m[i], g, ITERS)
                for block in range(ITERS):
                    tile = jnp.where(group == block, place(shifted_m[i + block], g, block), tile)
                tiles.append(tile)
        early = (ITERS - 1) * packed
        for p in range(early):
            tiles = eliminate_panel(tiles, p)
        (final,) = add_finish(step, ITERS - 1)
        for g in range(packed):
            at_end = jnp.where(group == ITERS - 1, SCALE * place(final, g, ITERS - 1), 0.0)
            tiles[early + g] = tiles[early + g] + at_end
        for p in range(early, ITERS * packed):
            tiles = eliminate_panel(tiles, p)
        solved = jnp.concatenate(tiles, axis=0)[:, ITERS * size : (ITERS + 1) * size]
        none = jnp.zeros((size, size), F32)
        take = jnp.concatenate([solved, none], axis=0)
        drop = jnp.concatenate([none, solved], axis=0)
        both = jnp.concatenate([take, -SCALE * (drop + SHIFT * take)], axis=1)
        high, low = halves(both)
        turned = jnp.concatenate([high.astype(F32), low.astype(F32)], axis=1).T.astype(BF16)
        turned = jnp.concatenate([turned, turned], axis=1)
        more = step + 1 < steps
        rim = Rim()
        pairs = sorted({c - c % 2 for c in edges})
        for n, c in enumerate(pairs + [c for c in range(0, count, 2) if c not in pairs]):
            out = jnp.dot(
                turned, basis[:, c * LANES : (c + 2) * LANES], preferred_element_type=F32
            )
            out = out[: 2 * size] + out[2 * size :]
            for i in range(2):
                l, x = divmod(c + i, tile_x)
                cols = slice(i * LANES, (i + 1) * LANES)
                change = out[:size, cols]
                v[l, x] = v[l, x] + change
                left = k0[l, x] + out[size:, cols]
                r[l, x] = left
                left = left + coef[8, c + i : c + i + 1, :] * change
                if c + i < tile_x:
                    after = jnp.minimum(step + 1, steps - 1)
                    here = slice((c + i) * LANES, (c + i + 1) * LANES)
                    left = left - (
                        inj[pl.ds(pl.multiple_of(after * size, size), size), here]
                        - inj[pl.ds(pl.multiple_of(step * size, size), size), here]
                    )
                k0[l, x] = left
                rim.add(c + i, left)
            if n + 1 == len(pairs):
                @pl.when(more)
                def _():
                    start(x_copies(k0, e + ITERS), gx, nx)

        @pl.when(more)
        def _():
            rim.send(e + ITERS)

        return carry

    lax.fori_loop(0, steps, time_step, 0)


def solve_grid(nx, ny, steps, layers, tile_x, volts, injected, coef):
    size = injected.shape[0] // steps
    halos = 1 + steps * ITERS
    packed = (2 * ITERS) * size * size // LANES
    field = (layers, tile_x, size, LANES)
    dma = pltpu.SemaphoreType.DMA
    return pl.pallas_call(
        functools.partial(grid_kernel, nx, ny, steps, layers, tile_x),
        out_shape=[jax.ShapeDtypeStruct(field, F32)] * 2,
        in_specs=[pl.BlockSpec(memory_space=pltpu.VMEM)] * 3,
        out_specs=[pl.BlockSpec(memory_space=pltpu.VMEM)] * 2,
        scratch_shapes=[
            pltpu.VMEM(field, F32),
            pltpu.VMEM(field, F32),
            pltpu.VMEM(field, F32),
            pltpu.VMEM((2 * (ITERS + 1) * size, layers * tile_x * LANES), BF16),
            pltpu.VMEM((halos, 2, layers, size, LANES), F32),
            pltpu.VMEM((halos, 2, size, LANES), F32),
            pltpu.VMEM((halos, 2, size, LANES), F32),
            pltpu.VMEM((steps, nx, packed, LANES), F32),
            pltpu.VMEM((steps, ny, packed, LANES), F32),
            dma((halos, 2)), dma((halos, 2)), dma((halos, 2)), dma((halos, 2)),
            dma((steps, ITERS, nx)), dma((steps, ITERS, nx)),
            dma((steps, ITERS, ny)), dma((steps, ITERS, ny)),
        ],
        compiler_params=pltpu.CompilerParams(
            collective_id=0, has_side_effects=True, vmem_limit_bytes=48 * 1024 * 1024
        ),
        name="grid",
    )(volts, injected, coef)


def shifted(x, axis):
    length = lax.axis_size(axis)
    return lax.ppermute(x, axis, [(i, i + 1) for i in range(length - 1)])


def body(volts, cap, cond_x, cond_y, via, waveforms, placement, cells, wave_ids, amps):
    nx, ny = lax.axis_size("gx"), lax.axis_size("gy")
    devices = nx * ny
    scenarios, layers, tile_x, tile_y = volts.shape
    steps = waveforms.shape[0] // scenarios
    capacity = 2 * cells.shape[0] // devices
    slots = bin_instances(devices, capacity, placement[:, 0], cells, wave_ids, amps)
    arrived = lax.all_to_all(
        slots.reshape(2, devices, capacity), ("gx", "gy"), split_axis=1, concat_axis=1, tiled=True
    )
    injected = inject(arrived, waveforms, tile_x * tile_y)
    rim_x = shifted(cond_x[:, -1:, :], "gx")
    rim_y = shifted(cond_y[:, :, -1:], "gy")
    x_low = jnp.concatenate([rim_x, cond_x[:, :-1, :]], axis=1)
    y_low = jnp.concatenate([rim_y, cond_y[:, :, :-1]], axis=2)
    via_low = jnp.concatenate([jnp.zeros_like(via[:1]), via[:-1]], axis=0)
    at_x = lax.broadcasted_iota(jnp.int32, cond_x.shape, 1) + lax.axis_index("gx") * tile_x
    at_y = lax.broadcasted_iota(jnp.int32, cond_y.shape, 2) + lax.axis_index("gy") * tile_y
    x_next = jnp.where(at_x == nx * tile_x - 1, 0.0, cond_x)
    y_next = jnp.where(at_y == ny * tile_y - 1, 0.0, cond_y)
    around = cond_x + x_low + cond_y + y_low + via + via_low
    coef = jnp.stack([cap + around, around, x_next, x_low, y_next, y_low, via, via_low]) / SCALE
    coef = jnp.concatenate([coef[:1] - SHIFT, coef[1:], cap[None]], axis=0)
    coef = coef.reshape(9, layers * tile_x, tile_y)
    out, residual = solve_grid(
        nx, ny, steps, layers, tile_x, volts.reshape(-1, tile_y), injected, coef
    )
    return out.transpose(2, 0, 1, 3), residual.transpose(2, 0, 1, 3)


def solution(mesh):
    grid = P(None, "gx", "gy")
    field = P(None, None, "gx", "gy")
    flat = P(("gx", "gy"))
    return jax.shard_map(
        body,
        mesh=mesh,
        in_specs=(field, grid, grid, grid, grid, P(), P(("gx", "gy"), None), flat, flat, flat),
        out_specs=(field, field),
        check_vma=False,
    )
```

```python
import functools

import jax
import jax.numpy as jnp
from jax import lax
from jax.experimental import pallas as pl
from jax.experimental.pallas import tpu as pltpu
from jax.sharding import PartitionSpec as P

ITERS = 3
SUBLANES = 8
SCALE = 6.0
SHIFT = 1.125
LANES = 128
MESH = pl.DeviceIdType.MESH
NT = (((1,), (1,)), ((), ()))
F32 = jnp.float32
BF16 = jnp.bfloat16


def rows_iota(rows, cols):
    return lax.broadcasted_iota(jnp.int32, (rows, cols), 0)


def ones(mask):
    return mask.astype(F32).astype(BF16)


def wide(ref, row, count):
    return jnp.concatenate([ref[pl.ds(row + i, 1), :] for i in range(count)], axis=1)


def across(tile, k):
    return jnp.broadcast_to(tile[:, k : k + 1], tile.shape)


def down(tile, a):
    return jnp.broadcast_to(tile[a : a + 1, :], tile.shape)


def eliminate_panel(tiles, p):
    tile, k = tiles[p], SUBLANES * p
    sub = rows_iota(SUBLANES, LANES)
    columns = [across(tile, k + b) for b in range(SUBLANES)]
    pivot = [[down(columns[b], a) for b in range(SUBLANES)] for a in range(SUBLANES)]
    right = [down(tile, a) for a in range(SUBLANES)]
    inverse = []
    for a in range(SUBLANES):
        inverse.append(1.0 / pivot[a][a])
        for b in range(a + 1, SUBLANES):
            factor = pivot[a][b] * inverse[a]
            right[b] = right[b] - factor * right[a]
            for c in range(b, SUBLANES):
                pivot[b][c] = pivot[b][c] - factor * pivot[a][c]
    solved = [None] * SUBLANES
    for a in reversed(range(SUBLANES)):
        row = right[a]
        for b in reversed(range(a + 1, SUBLANES)):
            row = row - pivot[a][b] * solved[b]
        solved[a] = row * inverse[a]
    fresh = []
    for i, other in enumerate(tiles):
        if i == p:
            result = solved[0]
            for a in range(1, SUBLANES):
                result = jnp.where(sub == a, solved[a], result)
        else:
            result = other
            for b in range(SUBLANES):
                result = result - across(other, k + b) * solved[b]
        fresh.append(result)
    return fresh


def halves(x):
    high = x.astype(BF16)
    return high, (x - high.astype(F32)).astype(BF16)


def grid_kernel(
    nx, ny, steps, layers, tile_x, capacity,
    v_hbm, cap_hbm, x_hbm, y_hbm, via_hbm, waves_hbm, target_hbm, cells_hbm, kinds_hbm, amps_hbm,
    v, r,
    v_in, cap, cond_x, cond_y, via, waves, target, cells, kinds, amps, isem,
    k0, k1, k2, basis, xl, ys, yl, gl, hl,
    coef, xc, yc, spots, bins, send, land, table, inj,
    xsend, xrecv, ysend, yrecv, gsend, grecv, hsend, hrecv, csend, crecv, asend, arecv,
):
    gx, gy = lax.axis_index("gx"), lax.axis_index("gy")
    size = xl.shape[3]
    count = layers * tile_x
    halos = 1 + ITERS * steps
    packed = LANES // size
    part = size // packed
    spans = ((0, 3 * part), (3 * part, 2 * part), (5 * part, part))
    lane = lax.broadcasted_iota(jnp.int32, (size, LANES), 1)
    group = lax.broadcasted_iota(jnp.int32, (part, LANES), 1) // size
    edges = [l * tile_x + x for l in range(layers) for x in (0, tile_x - 1)]
    inner = [c for c in range(count) if c not in edges]
    fields = (k0, k1, k2)
    devices = nx * ny
    low_count = inj.shape[2]
    high_count = inj.shape[1] // size
    kind_count = waves.shape[1]
    lane_count = bins.shape[1]
    rows_a_plane = capacity // LANES

    def at(ref, c):
        return ref.at[c // tile_x, c % tile_x]

    def x_copies(src, e):
        return [
            pltpu.make_async_remote_copy(
                src.at[:, tile_x - 1 if side == 0 else 0], xl.at[e, side],
                xsend.at[e, side], xrecv.at[e, side],
                device_id={"gx": lax.rem(gx + (1 if side == 0 else nx - 1), nx)},
                device_id_type=MESH,
            )
            for side in range(2)
        ]

    def y_copies(e):
        return [
            pltpu.make_async_remote_copy(
                ys.at[e, side], yl.at[e, side], ysend.at[e, side], yrecv.at[e, side],
                device_id={"gy": lax.rem(gy + (1 if side == 0 else ny - 1), ny)},
                device_id_type=MESH,
            )
            for side in range(2)
        ]

    def start(copies, me, n):
        pl.when(me < n - 1)(copies[0].start)
        pl.when(me > 0)(copies[1].start)

    def finish(copies, me, n):
        @pl.when(me > 0)
        def _():
            copies[0].wait_recv()
            copies[1].wait_send()

        @pl.when(me < n - 1)
        def _():
            copies[1].wait_recv()
            copies[0].wait_send()

    def arrive(src, e):
        finish(x_copies(src, e), gx, nx)
        finish(y_copies(e), gy, ny)

    class Rim:
        def __init__(self):
            self.last = jnp.zeros((size, LANES), F32)
            self.first = self.last

        def add(self, c, f):
            self.last = jnp.where(lane == c, pltpu.roll(f, (c + 1) % LANES, 1), self.last)
            self.first = jnp.where(lane == c, pltpu.roll(f, c, 1) if c else f, self.first)

        def send(self, e):
            ys[e, 0] = self.last
            ys[e, 1] = self.first
            start(y_copies(e), gy, ny)

    def stencil(src, e, own, emit, after_edges):
        y_low, y_high = yl[e, 0], yl[e, 1]
        for n, c in enumerate(edges + inner):
            l, x = divmod(c, tile_x)
            f = src[l, x]

            def k(i):
                return coef[i, c : c + 1, :]

            high = src[l, x + 1] if x + 1 < tile_x else xl[e, 1, l]
            low = src[l, x - 1] if x else xl[e, 0, l]
            total = k(own) * f - k(2) * high - k(3) * low
            after = jnp.where(
                lane == LANES - 1, pltpu.roll(y_high, LANES - 1 - c, 1), pltpu.roll(f, LANES - 1, 1)
            )
            ahead = jnp.where(
                lane == 0, pltpu.roll(y_low, LANES - c, 1) if c else y_low, pltpu.roll(f, 1, 1)
            )
            total = total - k(4) * after - k(5) * ahead
            if l + 1 < layers:
                total = total - k(6) * src[l + 1, x]
            if l:
                total = total - k(7) * src[l - 1, x]
            emit(c, total)
            if n + 1 == len(edges):
                after_edges()

    def split(j, c, f):
        high, low = halves(f)
        cols = slice(c * LANES, (c + 1) * LANES)
        basis[j * size : (j + 1) * size, cols] = high
        basis[(ITERS + 1 + j) * size : (ITERS + 2 + j) * size, cols] = low

    def grams(left, j):
        def rows(i):
            return [basis[b * size : (b + 1) * size, :] for b in (i, ITERS + 1 + i)]

        every = [block for i in left for block in rows(i)]
        product = lax.dot_general(
            jnp.concatenate(every, axis=0), jnp.concatenate(rows(j), axis=0), NT,
            preferred_element_type=F32,
        )
        product = product[:, :size] + product[:, size:]
        return [
            product[2 * i * size : (2 * i + 1) * size] + product[(2 * i + 1) * size : (2 * i + 2) * size]
            for i in range(len(left))
        ]

    def pack(matrix):
        return jnp.concatenate([matrix[i * part : (i + 1) * part] for i in range(packed)], axis=1)

    def gather(land, step, g, ssem, rsem, axis, me, n):
        rows = pl.ds(spans[g][0], spans[g][1])
        return [
            pltpu.make_async_remote_copy(
                land.at[step, me, rows], land.at[step, me, rows],
                ssem.at[step, g, j], rsem.at[step, g, j],
                device_id={axis: lax.rem(me + j, n)}, device_id_type=MESH,
            )
            for j in range(1, n)
        ]

    def along_x(step, g):
        return gather(gl, step, g, gsend, grecv, "gx", gx, nx)

    def along_y(step, g):
        return gather(hl, step, g, hsend, hrecv, "gy", gy, ny)

    def add_start(step, g, matrices):
        for i, matrix in enumerate(matrices):
            gl[step, gx, pl.ds(spans[g][0] + i * part, part), :] = pack(matrix)
        for copy in along_x(step, g):
            copy.start()

    def landed(land, copies, step, g, n):
        for copy in copies:
            copy.wait()
        first, rows = spans[g]
        total = land[step, 0, first : first + rows, :]
        for j in range(1, n):
            total = total + land[step, j, first : first + rows, :]
        return total

    def add_turn(step, g):
        total = landed(gl, along_x(step, g), step, g, nx)
        hl[step, gy, pl.ds(*spans[g]), :] = total
        for copy in along_y(step, g):
            copy.start()

    def add_finish(step, g):
        total = landed(hl, along_y(step, g), step, g, ny)
        return [total[i * part : (i + 1) * part] for i in range(spans[g][1] // part)]

    def place(matrix, g, block):
        shift = ((block - g) * size) % LANES
        return pltpu.roll(matrix, shift, 1) if shift else matrix

    def rim_copies():
        return [
            pltpu.make_async_remote_copy(
                from_ref, to_ref, csend.at[i], crecv.at[i],
                device_id={axis: lax.rem(me + 1, n)}, device_id_type=MESH,
            )
            for i, (from_ref, to_ref, axis, me, n) in enumerate(
                ((cond_x, xc, "gx", gx, nx), (cond_y, yc, "gy", gy, ny))
            )
        ]

    def coefficients():
        row = rows_iota(tile_x, LANES)
        col = lax.broadcasted_iota(jnp.int32, (tile_x, LANES), 1)
        above = jnp.zeros((tile_x, LANES), F32)
        for l in range(layers):
            at = slice(l * tile_x, (l + 1) * tile_x)
            x_low = jnp.where(row == 0, pltpu.roll(xc[at], 1, 0), pltpu.roll(cond_x[at], 1, 0))
            y_low = jnp.where(col == 0, pltpu.roll(yc[at], 1, 1), pltpu.roll(cond_y[at], 1, 1))
            x_end = jnp.logical_and(row == tile_x - 1, gx == nx - 1)
            y_end = jnp.logical_and(col == LANES - 1, gy == ny - 1)
            around = cond_x[at] + x_low + cond_y[at] + y_low + via[at] + above
            values = [
                (cap[at] + around) / SCALE - SHIFT, around / SCALE,
                jnp.where(x_end, 0.0, cond_x[at]) / SCALE, x_low / SCALE,
                jnp.where(y_end, 0.0, cond_y[at]) / SCALE, y_low / SCALE,
                via[at] / SCALE, above / SCALE, cap[at],
            ]
            for i, value in enumerate(values):
                coef[i, at] = value
            above = via[at]

    def find_spots():
        width = 2 * LANES
        before = ones(rows_iota(width, width) < lax.broadcasted_iota(jnp.int32, (width, width), 1))
        together = 4

        def body(q, base):
            hits = [
                (rows_iota(devices, width) == wide(target, (q * together + i) * 2, 2)).astype(F32)
                for i in range(together)
            ]
            ahead = jnp.dot(
                jnp.concatenate(hits, axis=0).astype(BF16), before, preferred_element_type=F32
            )
            for i, hit in enumerate(hits):
                count = ahead[i * devices : (i + 1) * devices]
                spot = jnp.sum(hit * (count + base), axis=0, keepdims=True).astype(jnp.int32)
                for half in range(2):
                    at = pl.ds((q * together + i) * 2 + half, 1)
                    spots[at, :] = spot[:, half * LANES : (half + 1) * LANES]
                base = base + jnp.broadcast_to((count + hit)[:, width - 1 :], base.shape)
            return base

        lax.fori_loop(
            0, target.shape[0] // (2 * together), body, jnp.zeros((devices, width), F32)
        )

    def fill_bins():
        rows = bins.shape[0] // 4
        width = 4 * LANES
        bins[...] = jnp.zeros_like(bins)

        def body(b, carry):
            spot = wide(spots, b * 4, 4)
            key = wide(target, b * 4, 4) + (spot // lane_count) * devices
            mask = rows_iota(rows, width) == key
            there = ones(rows_iota(lane_count, width) == spot % lane_count)
            code = wide(cells, b * 4, 4) * kind_count + wide(kinds, b * 4, 4)
            amp = wide(amps, b * 4, 4)
            amp_high = amp.astype(BF16).astype(F32)
            parts = (amp_high, amp - amp_high, (code >> 8).astype(F32), (code & 255).astype(F32))
            left = jnp.concatenate([jnp.where(mask, p, 0.0).astype(BF16) for p in parts], axis=0)
            bins[...] += lax.dot_general(left, there, NT, preferred_element_type=F32)
            return carry

        lax.fori_loop(0, target.shape[0] // 4, body, 0, unroll=2)
        planes = (
            bins[:rows] + bins[rows : 2 * rows],
            bins[2 * rows : 3 * rows] * 256.0 + bins[3 * rows :],
        )
        if 2 * rows_a_plane < SUBLANES:
            send[...] = jnp.zeros_like(send)
        for i, plane in enumerate(planes):
            for row in range(rows_a_plane):
                first, col = divmod(row * LANES, lane_count)
                send[pl.ds(i * rows_a_plane + row, devices, stride=SUBLANES), :] = plane[
                    first * devices : (first + 1) * devices, col : col + LANES
                ]

    def bin_copy(j):
        to_x = lax.rem(gx + j // ny, nx)
        to_y = lax.rem(gy + j % ny, ny)
        at = pl.multiple_of((to_x * ny + to_y) * SUBLANES, SUBLANES)
        return pltpu.make_async_remote_copy(
            send.at[pl.ds(at, SUBLANES)], land.at[j], asend.at[j], arecv.at[j],
            device_id={"gx": to_x, "gy": to_y}, device_id_type=MESH,
        )

    def inject(step, j):
        width = capacity
        amp = wide(land.at[j], 0, rows_a_plane)
        code = wide(land.at[j], rows_a_plane, rows_a_plane).astype(jnp.int32)
        cell = code // kind_count
        kind_hits = ones(rows_iota(kind_count, width) == code % kind_count)
        picked = jnp.dot(table[step], kind_hits, preferred_element_type=F32)
        currents = ((picked[:size] + picked[size:]) * amp).astype(BF16).astype(F32)
        high = cell // low_count
        left = jnp.concatenate(
            [jnp.where(high == h, currents, 0.0).astype(BF16) for h in range(high_count)], axis=0
        )
        low_hits = ones(rows_iota(low_count, width) == cell % low_count)
        inj[step] += lax.dot_general(left, low_hits, NT, preferred_element_type=F32)

    def injected(step, c):
        h, col = divmod(c * LANES, low_count)
        return inj[step, h * size : (h + 1) * size, col : col + LANES]

    together = 4

    def inject_part(step, part, parts):
        each = devices // parts

        def body(q, carry):
            for i in range(together):
                inject(step, part * each + q * together + i)
            return carry

        lax.fori_loop(0, each // together, body, 0)

    inputs = [
        pltpu.make_async_copy(outside, inside, isem.at[i])
        for i, (outside, inside) in enumerate((
            (target_hbm, target), (v_hbm, v_in), (x_hbm, cond_x), (y_hbm, cond_y),
            (cells_hbm, cells), (kinds_hbm, kinds), (amps_hbm, amps),
            (waves_hbm, waves), (cap_hbm, cap), (via_hbm, via),
        ))
    ]
    for copy in inputs:
        copy.start()
    for e in range(halos):
        for me, n, to in ((gx, nx, xl), (gy, ny, yl)):
            for side, last in ((0, 0), (1, n - 1)):
                @pl.when(me == last)
                def _():
                    to[e, side] = jnp.zeros(to.shape[2:], F32)

    @pl.when(gx == 0)
    def _():
        xc[...] = jnp.zeros_like(xc)

    @pl.when(gy == 0)
    def _():
        yc[...] = jnp.zeros_like(yc)

    barrier = pltpu.get_barrier_semaphore()

    def greet(j, carry):
        pl.semaphore_signal(
            barrier, inc=1,
            device_id={"gx": lax.rem(gx + j // ny, nx), "gy": lax.rem(gy + j % ny, ny)},
            device_id_type=MESH,
        )
        return carry

    lax.fori_loop(1, devices, greet, 0)
    inputs[0].wait()
    find_spots()
    inputs[1].wait()
    rim = Rim()
    for c in range(count):
        f = v_in[pl.ds(c, size, stride=count), :]
        k1[c // tile_x, c % tile_x] = f
        v[pl.ds(c, size, stride=count), :] = f
        rim.add(c, f)
    for copy in inputs[2:]:
        copy.wait()
    pl.semaphore_wait(barrier, devices - 1)
    start(x_copies(k1, 0), gx, nx)
    rim.send(0)
    rims = rim_copies()
    pl.when(gx < nx - 1)(rims[0].start)
    pl.when(gy < ny - 1)(rims[1].start)
    fill_bins()

    def start_bin(j, carry):
        bin_copy(j).start()
        return carry

    lax.fori_loop(1, devices, start_bin, 0)
    own = pl.multiple_of((gx * ny + gy) * SUBLANES, SUBLANES)
    land[0] = send[pl.ds(own, SUBLANES), :]
    wave_high, wave_low = halves(waves[...])
    for step in range(steps):
        at = slice(step * size, (step + 1) * size)
        table[step, :size] = wave_high[at]
        table[step, size:] = wave_low[at]
    inj[...] = jnp.zeros_like(inj)
    arrive(k1, 0)
    for i, (me, n) in enumerate(((gx, nx), (gy, ny))):
        pl.when(me > 0)(rims[i].wait_recv)
        pl.when(me < n - 1)(rims[i].wait_send)
    coefficients()
    rim = Rim()

    def first_residual(c, total):
        f = -SCALE * total
        k0[c // tile_x, c % tile_x] = f
        if c >= tile_x:
            rim.add(c, f)

    stencil(k1, 0, 1, first_residual, lambda: None)

    def first_inject(q, carry):
        for i in range(together):
            j = q * together + i
            if i:
                bin_copy(j).wait()
            else:
                pl.when(j > 0)(bin_copy(j).wait)
        for i in range(together):
            inject(0, q * together + i)
        return carry

    lax.fori_loop(0, devices // together, first_inject, 0)
    for c in range(tile_x):
        f = k0[0, c] - injected(0, c)
        k0[0, c] = f
        rim.add(c, f)
    start(x_copies(k0, 1), gx, nx)
    rim.send(1)

    def time_step(step, carry):
        e = 1 + ITERS * step
        more = step + 1 < steps

        def inject_next(part):
            @pl.when(more)
            def _():
                inject_part(step + 1, part, ITERS + 1)

        for c in range(count):
            split(0, c, k0[c // tile_x, c % tile_x])
        moments = grams([0], 0)
        inject_next(0)
        for j in range(1, ITERS + 1):
            arrive(fields[j - 1], e + j - 1)
            if j > 1:
                add_turn(step, j - 2)
            rim = Rim()

            def next_field(c, total):
                split(j, c, total)
                if j < ITERS:
                    fields[j][c // tile_x, c % tile_x] = total
                    rim.add(c, total)

            def send_edges():
                if j < ITERS:
                    start(x_copies(fields[j], e + j), gx, nx)

            stencil(fields[j - 1], e + j - 1, 0, next_field, send_edges)
            if j < ITERS:
                rim.send(e + j)
            moments = moments + grams([j - 1, j] if j < ITERS else [j - 1], j)
            add_start(step, j - 1, moments)
            moments = []
            inject_next(j)
        m = add_finish(step, 0)
        add_turn(step, ITERS - 1)
        m = m + add_finish(step, 1)
        m.append(jnp.zeros_like(m[0]))
        shifted_m = [SCALE * (m[i + 1] + SHIFT * m[i]) for i in range(len(m) - 1)]
        tiles = []
        for i in range(ITERS):
            for g in range(packed):
                tile = place(m[i], g, ITERS)
                for block in range(ITERS):
                    tile = jnp.where(group == block, place(shifted_m[i + block], g, block), tile)
                tiles.append(tile)
        early = (ITERS - 1) * packed
        for p in range(early):
            tiles = eliminate_panel(tiles, p)
        (final,) = add_finish(step, ITERS - 1)
        for g in range(packed):
            at_end = jnp.where(group == ITERS - 1, SCALE * place(final, g, ITERS - 1), 0.0)
            tiles[early + g] = tiles[early + g] + at_end
        for p in range(early, ITERS * packed):
            tiles = eliminate_panel(tiles, p)
        solved = jnp.concatenate(tiles, axis=0)[:, ITERS * size : (ITERS + 1) * size]
        none = jnp.zeros((size, size), F32)
        take = jnp.concatenate([solved, none], axis=0)
        drop = jnp.concatenate([none, solved], axis=0)
        both = jnp.concatenate([take, -SCALE * (drop + SHIFT * take)], axis=1)
        high, low = halves(both)
        turned = jnp.concatenate([high.astype(F32), low.astype(F32)], axis=1).T.astype(BF16)
        turned = jnp.concatenate([turned, turned], axis=1)
        rim = Rim()
        pairs = sorted({c - c % 2 for c in edges})
        for n, c in enumerate(pairs + [c for c in range(0, count, 2) if c not in pairs]):
            out = jnp.dot(
                turned, basis[:, c * LANES : (c + 2) * LANES], preferred_element_type=F32
            )
            out = out[: 2 * size] + out[2 * size :]
            for i in range(2):
                l, x = divmod(c + i, tile_x)
                cols = slice(i * LANES, (i + 1) * LANES)
                change = out[:size, cols]
                rows = pl.ds(c + i, size, stride=count)
                v[rows, :] = v[rows, :] + change
                left = k0[l, x] + out[size:, cols]
                r[rows, :] = left
                left = left + coef[8, c + i : c + i + 1, :] * change
                if c + i < tile_x:
                    after = jnp.minimum(step + 1, steps - 1)
                    left = left - (injected(after, c + i) - injected(step, c + i))
                k0[l, x] = left
                rim.add(c + i, left)
            if n + 1 == len(pairs):
                @pl.when(more)
                def _():
                    start(x_copies(k0, e + ITERS), gx, nx)

        @pl.when(more)
        def _():
            rim.send(e + ITERS)

        return carry

    lax.fori_loop(0, steps, time_step, 0)


def body(volts, cap, cond_x, cond_y, via, waveforms, placement, cells, wave_ids, amps):
    nx, ny = lax.axis_size("gx"), lax.axis_size("gy")
    devices = nx * ny
    size, layers, tile_x, tile_y = volts.shape
    steps = waveforms.shape[0] // size
    count = layers * tile_x
    capacity = 2 * cells.shape[0] // devices
    lane_count = min(capacity, 2 * LANES)
    halos = 1 + steps * ITERS
    packed = (2 * ITERS) * size * size // LANES
    low_count = 2 * LANES
    high_count = tile_x * tile_y // low_count
    field = (layers, tile_x, size, LANES)
    dma = pltpu.SemaphoreType.DMA
    flat = (count, tile_y)
    many = (cells.shape[0] // LANES, LANES)
    out, residual = pl.pallas_call(
        functools.partial(grid_kernel, nx, ny, steps, layers, tile_x, capacity),
        out_shape=[jax.ShapeDtypeStruct((size * count, LANES), F32)] * 2,
        in_specs=[pl.BlockSpec(memory_space=pltpu.HBM)] * 10,
        out_specs=[pl.BlockSpec(memory_space=pltpu.VMEM)] * 2,
        scratch_shapes=[
            pltpu.VMEM((size * count, LANES), F32),
            *[pltpu.VMEM(flat, F32)] * 4,
            pltpu.VMEM(waveforms.shape, F32),
            *[pltpu.VMEM(many, jnp.int32)] * 3,
            pltpu.VMEM(many, F32),
            dma((10,)),
            pltpu.VMEM(field, F32),
            pltpu.VMEM(field, F32),
            pltpu.VMEM(field, F32),
            pltpu.VMEM((2 * (ITERS + 1) * size, count * LANES), BF16),
            pltpu.VMEM((halos, 2, layers, size, LANES), F32),
            pltpu.VMEM((halos, 2, size, LANES), F32),
            pltpu.VMEM((halos, 2, size, LANES), F32),
            pltpu.VMEM((steps, nx, packed, LANES), F32),
            pltpu.VMEM((steps, ny, packed, LANES), F32),
            pltpu.VMEM((9,) + flat, F32),
            pltpu.VMEM(flat, F32),
            pltpu.VMEM(flat, F32),
            pltpu.VMEM(many, jnp.int32),
            pltpu.VMEM((4 * devices * capacity // lane_count, lane_count), F32),
            pltpu.VMEM((devices * SUBLANES, LANES), F32),
            pltpu.VMEM((devices, SUBLANES, LANES), F32),
            pltpu.VMEM((steps, 2 * size, waveforms.shape[1]), BF16),
            pltpu.VMEM((steps, high_count * size, low_count), F32),
            dma((halos, 2)), dma((halos, 2)), dma((halos, 2)), dma((halos, 2)),
            dma((steps, ITERS, nx)), dma((steps, ITERS, nx)),
            dma((steps, ITERS, ny)), dma((steps, ITERS, ny)),
            dma((2,)), dma((2,)), dma((devices,)), dma((devices,)),
        ],
        compiler_params=pltpu.CompilerParams(
            collective_id=0, has_side_effects=True, vmem_limit_bytes=67043328
        ),
        name="transient",
    )(
        volts.reshape(-1, tile_y),
        *[x.reshape(flat) for x in (cap, cond_x, cond_y, via)],
        waveforms,
        *[x.reshape(many) for x in (placement, cells, wave_ids, amps)],
    )
    return out.reshape(volts.shape), residual.reshape(volts.shape)


def solution(mesh):
    grid = P(None, "gx", "gy")
    field = P(None, None, "gx", "gy")
    flat = P(("gx", "gy"))
    return jax.shard_map(
        body,
        mesh=mesh,
        in_specs=(field, grid, grid, grid, grid, P(), P(("gx", "gy"), None), flat, flat, flat),
        out_specs=(field, field),
        check_vma=False,
    )
```

```python
import functools

import jax
import jax.numpy as jnp
from jax import lax
from jax.experimental import pallas as pl
from jax.experimental.pallas import tpu as pltpu
from jax.sharding import PartitionSpec as P

ITERS = 3
SUBLANES = 8
SCALE = 6.0
SHIFT = 1.125
LANES = 128
MESH = pl.DeviceIdType.MESH
NT = (((1,), (1,)), ((), ()))
F32 = jnp.float32
BF16 = jnp.bfloat16


def rows_iota(rows, cols):
    return lax.broadcasted_iota(jnp.int32, (rows, cols), 0)


def ones(mask):
    return mask.astype(F32).astype(BF16)


def picks(row, count):
    lines = rows_iota(count, row.shape[1]).astype(F32).astype(BF16)
    return jnp.where(lines == packed_row(row, count), BF16(1), BF16(0))


def packed_row(row, count):
    once = jnp.broadcast_to(row.astype(F32), (2 * SUBLANES, row.shape[1])).astype(BF16)
    return jnp.concatenate([once] * (count // (2 * SUBLANES)), axis=0)


def parted(x, count):
    return x >> (count.bit_length() - 1), x & (count - 1)


def wide(ref, row, count):
    return jnp.concatenate([ref[pl.ds(row + i, 1), :] for i in range(count)], axis=1)


def across(tile, k):
    return jnp.broadcast_to(tile[:, k : k + 1], tile.shape)


def down(tile, a):
    return jnp.broadcast_to(tile[a : a + 1, :], tile.shape)


def eliminate_panel(tiles, p):
    tile, k = tiles[p], SUBLANES * p
    sub = rows_iota(SUBLANES, LANES)
    columns = [across(tile, k + b) for b in range(SUBLANES)]
    pivot = [[down(columns[b], a) for b in range(SUBLANES)] for a in range(SUBLANES)]
    right = [down(tile, a) for a in range(SUBLANES)]
    inverse = []
    for a in range(SUBLANES):
        inverse.append(1.0 / pivot[a][a])
        for b in range(a + 1, SUBLANES):
            factor = pivot[a][b] * inverse[a]
            right[b] = right[b] - factor * right[a]
            for c in range(b, SUBLANES):
                pivot[b][c] = pivot[b][c] - factor * pivot[a][c]
    solved = [None] * SUBLANES
    for a in reversed(range(SUBLANES)):
        row = right[a]
        for b in reversed(range(a + 1, SUBLANES)):
            row = row - pivot[a][b] * solved[b]
        solved[a] = row * inverse[a]
    fresh = []
    for i, other in enumerate(tiles):
        if i == p:
            result = solved[0]
            for a in range(1, SUBLANES):
                result = jnp.where(sub == a, solved[a], result)
        else:
            result = other
            for b in range(SUBLANES):
                result = result - across(other, k + b) * solved[b]
        fresh.append(result)
    return fresh


def halves(x):
    high = x.astype(BF16)
    return high, (x - high.astype(F32)).astype(BF16)


def grid_kernel(
    nx, ny, steps, layers, tile_x, capacity,
    v_hbm, cap_hbm, x_hbm, y_hbm, via_hbm, waves_hbm, target_hbm, cells_hbm, kinds_hbm, amps_hbm,
    v_out, r_out,
    v, r, cap, cond_x, cond_y, via, waves, target, cells, kinds, amps, isem, vsem, osem,
    k0, k1, k2, k3, basis, xl, ys, yl, gl, hl, al,
    coef, xc, yc, spots, bins, send, land, table, inj,
    xsend, xrecv, ysend, yrecv, gsend, grecv, hsend, hrecv, csend, crecv, asend, arecv, fsend, frecv,
):
    gx, gy = lax.axis_index("gx"), lax.axis_index("gy")
    size = xl.shape[3]
    count = layers * tile_x
    halos = 1 + ITERS * steps
    packed = LANES // size
    part = size // packed
    spans = ((0, 3 * part), (3 * part, 2 * part))
    lane = lax.broadcasted_iota(jnp.int32, (size, LANES), 1)
    group = lax.broadcasted_iota(jnp.int32, (part, LANES), 1) // size
    edges = [l * tile_x + x for l in range(layers) for x in (0, tile_x - 1)]
    inner = [c for c in range(count) if c not in edges]
    fields = (k0, k1, k2, k3)
    devices = nx * ny
    low_count = inj.shape[2]
    high_count = inj.shape[1] // size
    kind_count = waves.shape[1]
    lane_count = bins.shape[1]
    rows_a_plane = capacity // LANES

    def xor(me, other, n):
        for bit in range(n.bit_length() - 1):
            power = 2**bit
            me = me + power * ((other // power) % 2) * (1 - 2 * ((me // power) % 2))
        return me

    def peer(j):
        return xor(gx, j % nx, nx), xor(gy, j // nx, ny)

    def x_copies(src, e):
        return [
            pltpu.make_async_remote_copy(
                src.at[:, tile_x - 1 if side == 0 else 0], xl.at[e, side],
                xsend.at[e, side], xrecv.at[e, side],
                device_id={"gx": lax.rem(gx + (1 if side == 0 else nx - 1), nx)},
                device_id_type=MESH,
            )
            for side in range(2)
        ]

    def y_copies(e):
        return [
            pltpu.make_async_remote_copy(
                ys.at[e], yl.at[e, side], ysend.at[e, side], yrecv.at[e, side],
                device_id={"gy": lax.rem(gy + (1 if side == 0 else ny - 1), ny)},
                device_id_type=MESH,
            )
            for side in range(2)
        ]

    def start(copies, me, n):
        pl.when(me < n - 1)(copies[0].start)
        pl.when(me > 0)(copies[1].start)

    def finish(copies, me, n):
        @pl.when(me > 0)
        def _():
            copies[0].wait_recv()
            copies[1].wait_send()

        @pl.when(me < n - 1)
        def _():
            copies[1].wait_recv()
            copies[0].wait_send()

    def arrive(src, e):
        finish(x_copies(src, e), gx, nx)
        finish(y_copies(e), gy, ny)

    class Rim:
        def __init__(self):
            self.both = jnp.zeros((size, LANES), F32)

        def add(self, c, f):
            self.both = jnp.where(lane // 2 == c, pltpu.roll(f, 2 * c + 1, 1), self.both)

        def send(self, e):
            ys[e] = self.both
            start(y_copies(e), gy, ny)

    def k(i, c):
        return coef[i, c : c + 1, :]

    def inside(src, own, dst):
        for c in range(count):
            l, x = divmod(c, tile_x)
            f = src[l, x]
            total = k(own, c) * f
            if x + 1 < tile_x:
                total = total - k(2, c) * src[l, x + 1]
            if x:
                total = total - k(3, c) * src[l, x - 1]
            total = total - k(4, c) * pltpu.roll(f, LANES - 1, 1) - k(5, c) * pltpu.roll(f, 1, 1)
            if l + 1 < layers:
                total = total - k(6, c) * src[l + 1, x]
            if l:
                total = total - k(7, c) * src[l - 1, x]
            dst[l, x] = total

    def outside(dst, e, emit, after_edges):
        rims = jnp.where(lane % 2 == 0, yl[e, 0], pltpu.roll(yl[e, 1], LANES - 2, 1))
        for n, c in enumerate(edges + inner):
            l, x = divmod(c, tile_x)
            moved = pltpu.roll(rims, LANES - 2 * c, 1) if c else rims
            total = dst[l, x] - k(8, c) * moved
            if x + 1 == tile_x:
                total = total - k(2, c) * xl[e, 1, l]
            if x == 0:
                total = total - k(3, c) * xl[e, 0, l]
            emit(c, total)
            if n + 1 == len(edges):
                after_edges()

    def split(j, c, f):
        high, low = halves(f)
        cols = slice(c * LANES, (c + 1) * LANES)
        basis[j * size : (j + 1) * size, cols] = high
        basis[(ITERS + 1 + j) * size : (ITERS + 2 + j) * size, cols] = low

    def grams(left, j):
        def rows(i):
            return [basis[b * size : (b + 1) * size, :] for b in (i, ITERS + 1 + i)]

        every = [block for i in left for block in rows(i)]
        product = lax.dot_general(
            jnp.concatenate(every, axis=0), jnp.concatenate(rows(j), axis=0), NT,
            preferred_element_type=F32,
        )
        product = product[:, :size] + product[:, size:]
        return [
            product[2 * i * size : (2 * i + 1) * size] + product[(2 * i + 1) * size : (2 * i + 2) * size]
            for i in range(len(left))
        ]

    def pack(matrix):
        return jnp.concatenate([matrix[i * part : (i + 1) * part] for i in range(packed)], axis=1)

    def gather(land, step, g, ssem, rsem, axis, me, n):
        rows = pl.ds(spans[g][0], spans[g][1])
        return [
            pltpu.make_async_remote_copy(
                land.at[step, me, rows], land.at[step, me, rows],
                ssem.at[step, g, j], rsem.at[step, g, j],
                device_id={axis: lax.rem(me + j, n)}, device_id_type=MESH,
            )
            for j in range(1, n)
        ]

    def along_x(step, g):
        return gather(gl, step, g, gsend, grecv, "gx", gx, nx)

    def along_y(step, g):
        return gather(hl, step, g, hsend, hrecv, "gy", gy, ny)

    def add_start(step, g, matrices):
        for i, matrix in enumerate(matrices):
            gl[step, gx, pl.ds(spans[g][0] + i * part, part), :] = pack(matrix)
        for copy in along_x(step, g):
            copy.start()

    def landed(land, copies, step, g, n):
        for copy in copies:
            copy.wait()
        first, rows = spans[g]
        total = land[step, 0, first : first + rows, :]
        for j in range(1, n):
            total = total + land[step, j, first : first + rows, :]
        return total

    def add_turn(step, g):
        total = landed(gl, along_x(step, g), step, g, nx)
        hl[step, gy, pl.ds(*spans[g]), :] = total
        for copy in along_y(step, g):
            copy.start()

    def add_finish(step, g):
        total = landed(hl, along_y(step, g), step, g, ny)
        return [total[i * part : (i + 1) * part] for i in range(spans[g][1] // part)]

    def every_copy(step, j):
        to_x, to_y = peer(j)
        me = gx * ny + gy
        return pltpu.make_async_remote_copy(
            al.at[step, me], al.at[step, me], fsend.at[step, j], frecv.at[step, j],
            device_id={"gx": to_x, "gy": to_y}, device_id_type=MESH,
        )

    def every_start(step, matrix):
        al[step, gx * ny + gy] = pack(matrix)

        def body(i, carry):
            every_copy(step, devices - 1 - i).start()
            return carry

        lax.fori_loop(0, devices - 1, body, 0)

    def every_finish(step):
        def body(j, carry):
            every_copy(step, j).wait()
            return carry

        lax.fori_loop(1, devices, body, 0)
        terms = [al[step, j] for j in range(devices)]
        while len(terms) > 1:
            terms = [a + b for a, b in zip(terms[::2], terms[1::2])]
        return terms[0]

    def place(matrix, g, block):
        shift = ((block - g) * size) % LANES
        return pltpu.roll(matrix, shift, 1) if shift else matrix

    def rim_copies():
        return [
            pltpu.make_async_remote_copy(
                from_ref, to_ref, csend.at[i], crecv.at[i],
                device_id={axis: lax.rem(me + 1, n)}, device_id_type=MESH,
            )
            for i, (from_ref, to_ref, axis, me, n) in enumerate(
                ((cond_x, xc, "gx", gx, nx), (cond_y, yc, "gy", gy, ny))
            )
        ]

    def coefficients():
        row = rows_iota(tile_x, LANES)
        col = lax.broadcasted_iota(jnp.int32, (tile_x, LANES), 1)
        above = jnp.zeros((tile_x, LANES), F32)
        for l in range(layers):
            at = slice(l * tile_x, (l + 1) * tile_x)
            x_low = jnp.where(row == 0, pltpu.roll(xc[at], 1, 0), pltpu.roll(cond_x[at], 1, 0))
            y_low = jnp.where(col == 0, pltpu.roll(yc[at], 1, 1), pltpu.roll(cond_y[at], 1, 1))
            x_end = jnp.logical_and(row == tile_x - 1, gx == nx - 1)
            y_end = jnp.logical_and(col == LANES - 1, gy == ny - 1)
            around = cond_x[at] + x_low + cond_y[at] + y_low + via[at] + above
            first, final = col == 0, col == LANES - 1
            y_next = jnp.where(y_end, 0.0, cond_y[at])
            values = [
                (cap[at] + around) / SCALE - SHIFT, around / SCALE,
                jnp.where(x_end, 0.0, cond_x[at]) / SCALE, x_low / SCALE,
                jnp.where(final, 0.0, y_next) / SCALE, jnp.where(first, 0.0, y_low) / SCALE,
                via[at] / SCALE, above / SCALE,
                jnp.where(final, y_next, jnp.where(first, y_low, 0.0)) / SCALE, cap[at],
            ]
            for i, value in enumerate(values):
                coef[i, at] = value
            above = via[at]

    def find_spots():
        width = 2 * LANES
        before = ones(rows_iota(width, width) < lax.broadcasted_iota(jnp.int32, (width, width), 1))
        together = 8

        def body(q, base):
            hits = [
                (rows_iota(devices, width) == wide(target, (q * together + i) * 2, 2)).astype(F32)
                for i in range(together)
            ]
            ahead = jnp.dot(
                jnp.concatenate(hits, axis=0).astype(BF16), before, preferred_element_type=F32
            )
            for i, hit in enumerate(hits):
                count = ahead[i * devices : (i + 1) * devices]
                spot = jnp.sum(hit * (count + base), axis=0, keepdims=True).astype(jnp.int32)
                for half in range(2):
                    at = pl.ds((q * together + i) * 2 + half, 1)
                    spots[at, :] = spot[:, half * LANES : (half + 1) * LANES]
                base = base + jnp.broadcast_to((count + hit)[:, width - 1 :], base.shape)
            return base

        lax.fori_loop(
            0, target.shape[0] // (2 * together), body, jnp.zeros((devices, width), F32)
        )

    def fill_bins():
        rows = bins.shape[0] // 4
        width = 4 * LANES
        each = 2
        bins[...] = jnp.zeros_like(bins)

        def one(b):
            upper, lower = parted(wide(spots, b * 4, 4), lane_count)
            key = wide(target, b * 4, 4) + upper * devices
            hits = rows_iota(rows, width).astype(F32).astype(BF16) == packed_row(key, rows)
            code = wide(cells, b * 4, 4) * kind_count + wide(kinds, b * 4, 4)
            amp = wide(amps, b * 4, 4)
            amp_high = amp.astype(BF16).astype(F32)
            parts = (amp_high, amp - amp_high, code >> 8, code & 255)
            left = [jnp.where(hits, packed_row(p, rows), BF16(0)) for p in parts]
            return jnp.concatenate(left, axis=0), picks(lower, lane_count)

        def body(b, carry):
            pairs = [one(b * each + i) for i in range(each)]
            left, there = (jnp.concatenate(x, axis=1) for x in zip(*pairs))
            bins[...] += lax.dot_general(left, there, NT, preferred_element_type=F32)
            return carry

        lax.fori_loop(0, target.shape[0] // (4 * each), body, 0, unroll=2)
        planes = (
            bins[:rows] + bins[rows : 2 * rows],
            bins[2 * rows : 3 * rows] * 256.0 + bins[3 * rows :],
        )
        if 2 * rows_a_plane < SUBLANES:
            send[...] = jnp.zeros_like(send)
        for i, plane in enumerate(planes):
            for row in range(rows_a_plane):
                first, col = divmod(row * LANES, lane_count)
                send[pl.ds(i * rows_a_plane + row, devices, stride=SUBLANES), :] = plane[
                    first * devices : (first + 1) * devices, col : col + LANES
                ]

    def bin_copy(j):
        to_x, to_y = peer(j)
        at = pl.multiple_of((to_x * ny + to_y) * SUBLANES, SUBLANES)
        return pltpu.make_async_remote_copy(
            send.at[pl.ds(at, SUBLANES)], land.at[j], asend.at[j], arecv.at[j],
            device_id={"gx": to_x, "gy": to_y}, device_id_type=MESH,
        )

    def inject(step, sources):
        def one(j):
            amp = wide(land.at[j], 0, rows_a_plane)
            code = wide(land.at[j], rows_a_plane, rows_a_plane).astype(jnp.int32)
            cell, kind = parted(code, kind_count)
            upper, lower = parted(cell, low_count)
            picked = jnp.dot(table[step], picks(kind, kind_count), preferred_element_type=F32)
            currents = ((picked[:size] + picked[size:]) * amp).astype(BF16)
            high = packed_row(upper, size)
            left = [jnp.where(high == BF16(h), currents, BF16(0)) for h in range(high_count)]
            return jnp.concatenate(left, axis=0), picks(lower, low_count)

        left, hits = (jnp.concatenate(x, axis=1) for x in zip(*[one(j) for j in sources]))
        inj[step] += lax.dot_general(left, hits, NT, preferred_element_type=F32)

    def injected(step, c):
        h, col = divmod(c * LANES, low_count)
        return inj[step, h * size : (h + 1) * size, col : col + LANES]

    together = 4

    def inject_part(step, part, parts):
        each = devices // parts

        def body(q, carry):
            inject(step, [part * each + q * together + i for i in range(together)])
            return carry

        lax.fori_loop(0, each // together, body, 0)

    inputs = [
        pltpu.make_async_copy(there, here, isem.at[i])
        for i, (there, here) in enumerate((
            (target_hbm, target), (cells_hbm, cells), (kinds_hbm, kinds), (amps_hbm, amps),
            (x_hbm, cond_x), (y_hbm, cond_y), (cap_hbm, cap), (via_hbm, via), (waves_hbm, waves),
        ))
    ]
    fetches = [
        pltpu.make_async_copy(v_hbm.at[:, c], v.at[c // tile_x, c % tile_x], vsem.at[c])
        for c in range(count)
    ]
    for copy in inputs[:4] + fetches + inputs[4:]:
        copy.start()
    for e in range(halos):
        for me, n, to in ((gx, nx, xl), (gy, ny, yl)):
            for side, last in ((0, 0), (1, n - 1)):
                @pl.when(me == last)
                def _():
                    to[e, side] = jnp.zeros(to.shape[2:], F32)

    @pl.when(gx == 0)
    def _():
        xc[...] = jnp.zeros_like(xc)

    @pl.when(gy == 0)
    def _():
        yc[...] = jnp.zeros_like(yc)

    barrier = pltpu.get_barrier_semaphore()

    def greet(j, carry):
        pl.semaphore_signal(
            barrier, inc=1,
            device_id={"gx": lax.rem(gx + j // ny, nx), "gy": lax.rem(gy + j % ny, ny)},
            device_id_type=MESH,
        )
        return carry

    lax.fori_loop(1, devices, greet, 0)
    inputs[0].wait()
    find_spots()
    for copy in inputs[1:4]:
        copy.wait()
    fill_bins()
    for copy in fetches + inputs[4:]:
        copy.wait()
    rim = Rim()
    for c in range(count):
        rim.add(c, v[c // tile_x, c % tile_x])
    pl.semaphore_wait(barrier, devices - 1)

    rims = rim_copies()
    pl.when(gx < nx - 1)(rims[0].start)
    pl.when(gy < ny - 1)(rims[1].start)

    def start_bin(i, carry):
        bin_copy(devices - 1 - i).start()
        return carry

    lax.fori_loop(0, devices - 1, start_bin, 0)
    start(x_copies(v, 0), gx, nx)
    rim.send(0)
    own = pl.multiple_of((gx * ny + gy) * SUBLANES, SUBLANES)
    land[0] = send[pl.ds(own, SUBLANES), :]
    wave_high, wave_low = halves(waves[...])
    for step in range(steps):
        at = slice(step * size, (step + 1) * size)
        table[step, :size] = wave_high[at]
        table[step, size:] = wave_low[at]
    inj[...] = jnp.zeros_like(inj)

    def first_inject(q, carry):
        for i in range(together):
            j = q * together + i
            if i:
                bin_copy(j).wait()
            else:
                pl.when(j > 0)(bin_copy(j).wait)
        inject(0, [q * together + i for i in range(together)])
        return carry

    for i, (me, n) in enumerate(((gx, nx), (gy, ny))):
        pl.when(me > 0)(rims[i].wait_recv)
        pl.when(me < n - 1)(rims[i].wait_send)
    coefficients()
    inside(v, 1, k0)
    early = nx // together
    lax.fori_loop(0, early, first_inject, 0)
    arrive(v, 0)
    rim = Rim()

    def first_residual(c, total):
        f = -SCALE * total
        k0[c // tile_x, c % tile_x] = f
        if c >= tile_x:
            split(0, c, f)
            rim.add(c, f)

    outside(k0, 0, first_residual, lambda: None)
    lax.fori_loop(early, devices // together, first_inject, 0)
    for c in range(tile_x):
        f = k0[0, c] - injected(0, c)
        k0[0, c] = f
        split(0, c, f)
        rim.add(c, f)
    start(x_copies(k0, 1), gx, nx)
    rim.send(1)

    def time_step(step, carry):
        e = 1 + ITERS * step
        more = step + 1 < steps

        def inject_next(part):
            @pl.when(more)
            def _():
                inject_part(step + 1, part, ITERS + 1)

        moments = grams([0], 0)
        inside(k0, 0, k1)
        inject_next(0)
        for j in range(1, ITERS + 1):
            arrive(fields[j - 1], e + j - 1)
            if j > 1:
                add_turn(step, j - 2)
            rim = Rim()

            def next_field(c, total):
                split(j, c, total)
                if j < ITERS:
                    fields[j][c // tile_x, c % tile_x] = total
                    rim.add(c, total)

            def send_edges():
                if j < ITERS:
                    start(x_copies(fields[j], e + j), gx, nx)

            outside(fields[j], e + j - 1, next_field, send_edges)
            if j < ITERS:
                rim.send(e + j)
                moments = moments + grams([j - 1, j], j)
                inside(fields[j], 0, fields[j + 1])
                add_start(step, j - 1, moments)
                moments = []
            else:
                every_start(step, grams([j - 1], j)[0])
            inject_next(j)
        m = add_finish(step, 0) + add_finish(step, 1)
        m.append(jnp.zeros_like(m[0]))
        shifted_m = [SCALE * (m[i + 1] + SHIFT * m[i]) for i in range(len(m) - 1)]
        tiles = []
        for i in range(ITERS):
            for g in range(packed):
                tile = place(m[i], g, ITERS)
                for block in range(ITERS):
                    tile = jnp.where(group == block, place(shifted_m[i + block], g, block), tile)
                tiles.append(tile)
        early = (ITERS - 1) * packed
        for p in range(early):
            tiles = eliminate_panel(tiles, p)
        last = every_finish(step)
        for g in range(packed):
            at_end = jnp.where(group == ITERS - 1, SCALE * place(last, g, ITERS - 1), 0.0)
            tiles[early + g] = tiles[early + g] + at_end
        for p in range(early, ITERS * packed):
            tiles = eliminate_panel(tiles, p)
        solved = jnp.concatenate(tiles, axis=0)[:, ITERS * size : (ITERS + 1) * size]
        none = jnp.zeros((size, size), F32)
        take = jnp.concatenate([solved, none], axis=0)
        drop = jnp.concatenate([none, solved], axis=0)
        both = jnp.concatenate([take, -SCALE * (drop + SHIFT * take)], axis=1)
        high, low = halves(both)
        turned = jnp.concatenate([high.astype(F32), low.astype(F32)], axis=1).T.astype(BF16)
        turned = jnp.concatenate([turned, turned], axis=1)
        rim = Rim()
        pairs = sorted({c - c % 2 for c in edges})
        for n, c in enumerate(pairs + [c for c in range(0, count, 2) if c not in pairs]):
            out = jnp.dot(
                turned, basis[:, c * LANES : (c + 2) * LANES], preferred_element_type=F32
            )
            out = out[: 2 * size] + out[2 * size :]
            for i in range(2):
                l, x = divmod(c + i, tile_x)
                cols = slice(i * LANES, (i + 1) * LANES)
                change = out[:size, cols]
                v[l, x] = v[l, x] + change
                left = k0[l, x] + out[size:, cols]
                r[l, x] = left
                left = left + k(9, c + i) * change
                if c + i < tile_x:
                    after = jnp.minimum(step + 1, steps - 1)
                    left = left - (injected(after, c + i) - injected(step, c + i))
                k0[l, x] = left
                split(0, c + i, left)
                rim.add(c + i, left)
            if n + 1 == len(pairs):
                @pl.when(more)
                def _():
                    start(x_copies(k0, e + ITERS), gx, nx)

        @pl.when(more)
        def _():
            rim.send(e + ITERS)

        return carry

    lax.fori_loop(0, steps, time_step, 0)
    stores = []
    for i, (here, there) in enumerate(((v, v_out), (r, r_out))):
        for c in range(count):
            stores.append(
                pltpu.make_async_copy(here.at[c // tile_x, c % tile_x], there.at[:, c], osem.at[i, c])
            )
            stores[-1].start()
    for copy in stores:
        copy.wait()


def hand_over_kernel(first, second, first_out, second_out, held, fetched, stored):
    pairs = ((first, first_out), (second, second_out))
    chunks = held.shape[1]
    each = first.shape[0] // chunks

    def fetch(i, n):
        return pltpu.make_async_copy(
            pairs[i][0].at[pl.ds(n * each, each)], held.at[i, n], fetched.at[i, n]
        )

    def store(i, n):
        return pltpu.make_async_copy(
            held.at[i, n], pairs[i][1].at[pl.ds(n * each, each)], stored.at[i, n]
        )

    order = [(i, n) for n in range(chunks) for i in range(2)]
    for where in order:
        fetch(*where).start()
    for where in order:
        fetch(*where).wait()
        store(*where).start()
    for where in order:
        store(*where).wait()


def hand_over(first, second):
    chunks = 4
    dma = pltpu.SemaphoreType.DMA
    return pl.pallas_call(
        hand_over_kernel,
        out_shape=[jax.ShapeDtypeStruct(first.shape, F32)] * 2,
        in_specs=[pl.BlockSpec(memory_space=pltpu.HBM)] * 2,
        out_specs=[pl.BlockSpec(memory_space=pltpu.HBM)] * 2,
        scratch_shapes=[
            pltpu.VMEM((2, chunks, first.shape[0] // chunks) + first.shape[1:], F32),
            dma((2, chunks)), dma((2, chunks)),
        ],
        compiler_params=pltpu.CompilerParams(vmem_limit_bytes=67043328),
        name="hand_over",
    )(first, second)


def body(volts, cap, cond_x, cond_y, via, waveforms, placement, cells, wave_ids, amps):
    nx, ny = lax.axis_size("gx"), lax.axis_size("gy")
    devices = nx * ny
    size, layers, tile_x, tile_y = volts.shape
    steps = waveforms.shape[0] // size
    count = layers * tile_x
    capacity = 2 * cells.shape[0] // devices
    lane_count = min(capacity, 2 * LANES)
    halos = 1 + steps * ITERS
    packed = (2 * ITERS - 1) * size * size // LANES
    low_count = 2 * LANES
    high_count = tile_x * tile_y // low_count
    field = (layers, tile_x, size, LANES)
    dma = pltpu.SemaphoreType.DMA
    flat = (count, tile_y)
    many = (cells.shape[0] // LANES, LANES)
    out, residual = pl.pallas_call(
        functools.partial(grid_kernel, nx, ny, steps, layers, tile_x, capacity),
        out_shape=[jax.ShapeDtypeStruct((size, count, LANES), F32)] * 2,
        in_specs=[pl.BlockSpec(memory_space=pltpu.HBM)] * 10,
        out_specs=[pl.BlockSpec(memory_space=pltpu.HBM)] * 2,
        scratch_shapes=[
            pltpu.VMEM(field, F32),
            pltpu.VMEM(field, F32),
            *[pltpu.VMEM(flat, F32)] * 4,
            pltpu.VMEM(waveforms.shape, F32),
            *[pltpu.VMEM(many, jnp.int32)] * 3,
            pltpu.VMEM(many, F32),
            dma((9,)), dma((count,)), dma((2, count)),
            pltpu.VMEM(field, F32),
            pltpu.VMEM(field, F32),
            pltpu.VMEM(field, F32),
            pltpu.VMEM(field, F32),
            pltpu.VMEM((2 * (ITERS + 1) * size, count * LANES), BF16),
            pltpu.VMEM((halos, 2, layers, size, LANES), F32),
            pltpu.VMEM((halos, size, LANES), F32),
            pltpu.VMEM((halos, 2, size, LANES), F32),
            pltpu.VMEM((steps, nx, packed, LANES), F32),
            pltpu.VMEM((steps, ny, packed, LANES), F32),
            pltpu.VMEM((steps, devices, size * size // LANES, LANES), F32),
            pltpu.VMEM((10,) + flat, F32),
            pltpu.VMEM(flat, F32),
            pltpu.VMEM(flat, F32),
            pltpu.VMEM(many, jnp.int32),
            pltpu.VMEM((4 * devices * capacity // lane_count, lane_count), F32),
            pltpu.VMEM((devices * SUBLANES, LANES), F32),
            pltpu.VMEM((devices, SUBLANES, LANES), F32),
            pltpu.VMEM((steps, 2 * size, waveforms.shape[1]), BF16),
            pltpu.VMEM((steps, high_count * size, low_count), F32),
            dma((halos, 2)), dma((halos, 2)), dma((halos, 2)), dma((halos, 2)),
            dma((steps, ITERS, nx)), dma((steps, ITERS, nx)),
            dma((steps, ITERS, ny)), dma((steps, ITERS, ny)),
            dma((2,)), dma((2,)), dma((devices,)), dma((devices,)),
            dma((steps, devices)), dma((steps, devices)),
        ],
        compiler_params=pltpu.CompilerParams(
            collective_id=0, has_side_effects=True, vmem_limit_bytes=67043328
        ),
        name="transient",
    )(
        volts.reshape(size, count, tile_y),
        *[x.reshape(flat) for x in (cap, cond_x, cond_y, via)],
        waveforms,
        *[x.reshape(many) for x in (placement, cells, wave_ids, amps)],
    )
    out, residual = hand_over(out, residual)
    return out.reshape(volts.shape), residual.reshape(volts.shape)


def solution(mesh):
    grid = P(None, "gx", "gy")
    field = P(None, None, "gx", "gy")
    flat = P(("gx", "gy"))
    return jax.shard_map(
        body,
        mesh=mesh,
        in_specs=(field, grid, grid, grid, grid, P(), P(("gx", "gy"), None), flat, flat, flat),
        out_specs=(field, field),
        check_vma=False,
    )
```

```python
import functools

import jax
import jax.numpy as jnp
from jax import lax
from jax.experimental import pallas as pl
from jax.experimental.pallas import tpu as pltpu
from jax.sharding import PartitionSpec as P

ITERS = 3
SUBLANES = 8
SCALE = 6.0
SHIFT = 1.125
LANES = 128
MESH = pl.DeviceIdType.MESH
NT = (((1,), (1,)), ((), ()))
F32 = jnp.float32
BF16 = jnp.bfloat16


def rows_iota(rows, cols):
    return lax.broadcasted_iota(jnp.int32, (rows, cols), 0)


def ones(mask):
    return mask.astype(F32).astype(BF16)


def picks(row, count):
    lines = rows_iota(count, row.shape[1]).astype(F32).astype(BF16)
    return jnp.where(lines == packed_row(row, count), BF16(1), BF16(0))


def packed_row(row, count):
    once = jnp.broadcast_to(row.astype(F32), (2 * SUBLANES, row.shape[1])).astype(BF16)
    return jnp.concatenate([once] * (count // (2 * SUBLANES)), axis=0)


def parted(x, count):
    return x >> (count.bit_length() - 1), x & (count - 1)


def wide(ref, row, count):
    return jnp.concatenate([ref[pl.ds(row + i, 1), :] for i in range(count)], axis=1)


def across(tile, k):
    return jnp.broadcast_to(tile[:, k : k + 1], tile.shape)


def down(tile, a):
    return jnp.broadcast_to(tile[a : a + 1, :], tile.shape)


def eliminate_panel(tiles, p):
    tile, k = tiles[p], SUBLANES * p
    sub = rows_iota(SUBLANES, LANES)
    columns = [across(tile, k + b) for b in range(SUBLANES)]
    pivot = [[down(columns[b], a) for b in range(SUBLANES)] for a in range(SUBLANES)]
    right = [down(tile, a) for a in range(SUBLANES)]
    inverse = []
    for a in range(SUBLANES):
        inverse.append(1.0 / pivot[a][a])
        for b in range(a + 1, SUBLANES):
            factor = pivot[a][b] * inverse[a]
            right[b] = right[b] - factor * right[a]
            for c in range(b, SUBLANES):
                pivot[b][c] = pivot[b][c] - factor * pivot[a][c]
    solved = [None] * SUBLANES
    for a in reversed(range(SUBLANES)):
        row = right[a]
        for b in reversed(range(a + 1, SUBLANES)):
            row = row - pivot[a][b] * solved[b]
        solved[a] = row * inverse[a]
    fresh = []
    for i, other in enumerate(tiles):
        if i == p:
            result = solved[0]
            for a in range(1, SUBLANES):
                result = jnp.where(sub == a, solved[a], result)
        else:
            result = other
            for b in range(SUBLANES):
                result = result - across(other, k + b) * solved[b]
        fresh.append(result)
    return fresh


def halves(x):
    high = x.astype(BF16)
    return high, (x - high.astype(F32)).astype(BF16)


def settle(ref, semaphore):
    pltpu.make_async_copy(ref, ref, semaphore).wait()


def grid_kernel(
    nx, ny, steps, layers, tile_x, capacity,
    v_hbm, cap_hbm, x_hbm, y_hbm, via_hbm, waves_hbm, target_hbm, cells_hbm, kinds_hbm, amps_hbm,
    v_out, r_out,
    v, r, cap, cond_x, cond_y, via, waves, target, cells, kinds, amps, isem, vsem, osem,
    k0, k1, k2, k3, basis, xs, xl, ys, yl, gl, hl, al,
    coef, xc, yc, spots, bins, send, land, table, inj,
    xsend, xrecv, ysend, yrecv, gsend, grecv, hsend, hrecv, csend, crecv, asend, arecv, fsend, frecv,
):
    gx, gy = lax.axis_index("gx"), lax.axis_index("gy")
    size = xs.shape[3]
    count = layers * tile_x
    halos = 1 + ITERS * steps
    packed = LANES // size
    part = size // packed
    spans = ((0, 3 * part), (3 * part, 2 * part))
    lane = lax.broadcasted_iota(jnp.int32, (size, LANES), 1)
    group = lax.broadcasted_iota(jnp.int32, (part, LANES), 1) // size
    edges = [l * tile_x + x for l in range(layers) for x in (0, tile_x - 1)]
    inner = [c for c in range(count) if c not in edges]
    fields = (k0, k1, k2, k3)
    devices = nx * ny
    low_count = inj.shape[2]
    high_count = inj.shape[1] // size
    kind_count = waves.shape[1]
    lane_count = bins.shape[1]
    rows_a_plane = capacity // LANES
    together = 4

    def walk(me, n):
        flips = [2**b * (1 - 2 * ((me // 2**b) % 2)) for b in range(n.bit_length() - 1)]
        places = [me]
        for flip in flips:
            places += [place + flip for place in places]
        return places

    walk_x, walk_y = walk(gx, nx), walk(gy, ny)

    def peer(j):
        return walk_x[j % nx], walk_y[j // nx]

    def x_copies(e):
        return [
            pltpu.make_async_remote_copy(
                xs.at[e, side], xl.at[e, side], xsend.at[e % 2, side], xrecv.at[e % 2, side],
                device_id={"gx": gx + (1 if side == 0 else -1)}, device_id_type=MESH,
            )
            for side in range(2)
        ]

    def y_copies(e):
        return [
            pltpu.make_async_remote_copy(
                ys.at[e], yl.at[e, side], ysend.at[e % 2, side], yrecv.at[e % 2, side],
                device_id={"gy": gy + (1 if side == 0 else -1)},
                device_id_type=MESH,
            )
            for side in range(2)
        ]

    def start(copies, me, n):
        pl.when(me < n - 1)(copies[0].start)
        pl.when(me > 0)(copies[1].start)

    def finish(copies, me, n):
        @pl.when(me > 0)
        def _():
            copies[0].wait_recv()
            copies[1].wait_send()

        @pl.when(me < n - 1)
        def _():
            copies[1].wait_recv()
            copies[0].wait_send()

    def arrive(e):
        finish(x_copies(e), gx, nx)
        finish(y_copies(e), gy, ny)

    class Rim:
        def __init__(self, e):
            self.e = e
            self.both = jnp.zeros((size, LANES), F32)

        def add(self, c, f):
            l, x = divmod(c, tile_x)
            for side, edge in ((0, tile_x - 1), (1, 0)):
                if x == edge:
                    xs[self.e, side, l] = f.astype(BF16)
            self.both = jnp.where(lane // 2 == c, pltpu.roll(f, 2 * c + 1, 1), self.both)

        def send_x(self):
            start(x_copies(self.e), gx, nx)

        def send_y(self):
            ys[self.e] = self.both
            start(y_copies(self.e), gy, ny)

    def k(i, c):
        return coef[i, c : c + 1, :]

    def inside(src, own, dst):
        for c in range(count):
            l, x = divmod(c, tile_x)
            f = src[l, x]
            total = k(own, c) * f
            if x + 1 < tile_x:
                total = total - k(2, c) * src[l, x + 1]
            if x:
                total = total - k(3, c) * src[l, x - 1]
            total = total - k(4, c) * pltpu.roll(f, LANES - 1, 1) - k(5, c) * pltpu.roll(f, 1, 1)
            if l + 1 < layers:
                total = total - k(6, c) * src[l + 1, x]
            if l:
                total = total - k(7, c) * src[l - 1, x]
            dst[l, x] = total

    def outside(dst, e, emit, after_edges):
        rims = jnp.where(lane % 2 == 0, yl[e, 0], pltpu.roll(yl[e, 1], LANES - 2, 1))
        for n, c in enumerate(edges + inner):
            l, x = divmod(c, tile_x)
            moved = pltpu.roll(rims, LANES - 2 * c, 1) if c else rims
            total = dst[l, x] - k(8, c) * moved
            if x + 1 == tile_x:
                total = total - k(2, c) * xl[e, 1, l].astype(F32)
            if x == 0:
                total = total - k(3, c) * xl[e, 0, l].astype(F32)
            emit(c, total)
            if n + 1 == len(edges):
                after_edges()

    def split(j, c, f):
        high, low = halves(f)
        cols = slice(c * LANES, (c + 1) * LANES)
        basis[j * size : (j + 1) * size, cols] = high
        basis[(ITERS + 1 + j) * size : (ITERS + 2 + j) * size, cols] = low

    def grams(left, j):
        def rows(i):
            return [basis[b * size : (b + 1) * size, :] for b in (i, ITERS + 1 + i)]

        every = [block for i in left for block in rows(i)]
        product = lax.dot_general(
            jnp.concatenate(every, axis=0), jnp.concatenate(rows(j), axis=0), NT,
            preferred_element_type=F32,
        )
        product = product[:, :size] + product[:, size:]
        return [
            product[2 * i * size : (2 * i + 1) * size] + product[(2 * i + 1) * size : (2 * i + 2) * size]
            for i in range(len(left))
        ]

    def pack(matrix):
        return jnp.concatenate([matrix[i * part : (i + 1) * part] for i in range(packed)], axis=1)

    def gather(land, step, g, ssem, rsem, axis, places):
        rows = pl.ds(spans[g][0], spans[g][1])
        return [
            pltpu.make_async_remote_copy(
                land.at[step, places[0], rows], land.at[step, places[0], rows],
                ssem.at[step, g], rsem.at[step, g],
                device_id={axis: places[j]}, device_id_type=MESH,
            )
            for j in range(1, len(places))
        ]

    def along_x(step, g):
        return gather(gl, step, g, gsend, grecv, "gx", walk_x)

    def along_y(step, g):
        return gather(hl, step, g, hsend, hrecv, "gy", walk_y)

    def add_start(step, g, matrices):
        for i, matrix in enumerate(matrices):
            gl[step, gx, pl.ds(spans[g][0] + i * part, part), :] = pack(matrix)
        for copy in along_x(step, g):
            copy.start()

    def landed(land, ssem, rsem, step, g, n):
        first, rows = spans[g]
        for semaphore in (ssem, rsem):
            settle(land.at[step, pl.ds(0, n - 1), pl.ds(first, rows)], semaphore.at[step, g])
        total = land[step, 0, first : first + rows, :]
        for j in range(1, n):
            total = total + land[step, j, first : first + rows, :]
        return total

    def add_turn(step, g):
        total = landed(gl, gsend, grecv, step, g, nx)
        hl[step, gy, pl.ds(*spans[g]), :] = total
        for copy in along_y(step, g):
            copy.start()

    def add_finish(step, g):
        total = landed(hl, hsend, hrecv, step, g, ny)
        return [total[i * part : (i + 1) * part] for i in range(spans[g][1] // part)]

    def every_copy(step, j):
        to_x, to_y = peer(j)
        me = gx * ny + gy
        return pltpu.make_async_remote_copy(
            al.at[step, me], al.at[step, me], fsend.at[step], frecv.at[step],
            device_id={"gx": to_x, "gy": to_y}, device_id_type=MESH,
        )

    def every_start(step, matrix):
        al[step, gx * ny + gy] = pack(matrix)
        for j in reversed(range(1, devices)):
            every_copy(step, j).start()

    def every_finish(step):
        for semaphore in (fsend, frecv):
            settle(al.at[step, pl.ds(0, devices - 1)], semaphore.at[step])
        terms = [al[step, j] for j in range(devices)]
        while len(terms) > 1:
            terms = [a + b for a, b in zip(terms[::2], terms[1::2])]
        return terms[0]

    def place(matrix, g, block):
        shift = ((block - g) * size) % LANES
        return pltpu.roll(matrix, shift, 1) if shift else matrix

    def rim_copies():
        return [
            pltpu.make_async_remote_copy(
                from_ref, to_ref, csend.at[i], crecv.at[i],
                device_id={axis: me + 1}, device_id_type=MESH,
            )
            for i, (from_ref, to_ref, axis, me, n) in enumerate(
                ((cond_x, xc, "gx", gx, nx), (cond_y, yc, "gy", gy, ny))
            )
        ]

    def coefficients():
        row = rows_iota(tile_x, LANES)
        col = lax.broadcasted_iota(jnp.int32, (tile_x, LANES), 1)
        above = jnp.zeros((tile_x, LANES), F32)
        for l in range(layers):
            at = slice(l * tile_x, (l + 1) * tile_x)
            x_low = jnp.where(row == 0, pltpu.roll(xc[at], 1, 0), pltpu.roll(cond_x[at], 1, 0))
            y_low = jnp.where(col == 0, pltpu.roll(yc[at], 1, 1), pltpu.roll(cond_y[at], 1, 1))
            x_end = jnp.logical_and(row == tile_x - 1, gx == nx - 1)
            y_end = jnp.logical_and(col == LANES - 1, gy == ny - 1)
            around = cond_x[at] + x_low + cond_y[at] + y_low + via[at] + above
            first, final = col == 0, col == LANES - 1
            y_next = jnp.where(y_end, 0.0, cond_y[at])
            values = [
                (cap[at] + around) / SCALE - SHIFT, around / SCALE,
                jnp.where(x_end, 0.0, cond_x[at]) / SCALE, x_low / SCALE,
                jnp.where(final, 0.0, y_next) / SCALE, jnp.where(first, 0.0, y_low) / SCALE,
                via[at] / SCALE, above / SCALE,
                jnp.where(final, y_next, jnp.where(first, y_low, 0.0)) / SCALE, cap[at],
            ]
            for i, value in enumerate(values):
                coef[i, at] = value
            above = via[at]

    def find_spots():
        width = 2 * LANES
        before = ones(rows_iota(width, width) < lax.broadcasted_iota(jnp.int32, (width, width), 1))
        together = 8

        def body(q, base):
            hits = [
                (rows_iota(devices, width) == wide(target, (q * together + i) * 2, 2)).astype(F32)
                for i in range(together)
            ]
            ahead = jnp.dot(
                jnp.concatenate(hits, axis=0).astype(BF16), before, preferred_element_type=F32
            )
            for i, hit in enumerate(hits):
                count = ahead[i * devices : (i + 1) * devices]
                spot = jnp.sum(hit * (count + base), axis=0, keepdims=True).astype(jnp.int32)
                for half in range(2):
                    at = pl.ds((q * together + i) * 2 + half, 1)
                    spots[at, :] = spot[:, half * LANES : (half + 1) * LANES]
                base = base + jnp.broadcast_to((count + hit)[:, width - 1 :], base.shape)
            return base

        lax.fori_loop(
            0, target.shape[0] // (2 * together), body, jnp.zeros((devices, width), F32)
        )

    def fill_bins():
        rows = bins.shape[0] // 4
        width = 4 * LANES
        each = 2
        bins[...] = jnp.zeros_like(bins)

        def one(b):
            upper, lower = parted(wide(spots, b * 4, 4), lane_count)
            key = wide(target, b * 4, 4) + upper * devices
            hits = rows_iota(rows, width).astype(F32).astype(BF16) == packed_row(key, rows)
            code = wide(cells, b * 4, 4) * kind_count + wide(kinds, b * 4, 4)
            amp = wide(amps, b * 4, 4)
            amp_high = amp.astype(BF16).astype(F32)
            parts = (amp_high, amp - amp_high, code >> 8, code & 255)
            left = [jnp.where(hits, packed_row(p, rows), BF16(0)) for p in parts]
            return jnp.concatenate(left, axis=0), picks(lower, lane_count)

        def body(b, carry):
            pairs = [one(b * each + i) for i in range(each)]
            left, there = (jnp.concatenate(x, axis=1) for x in zip(*pairs))
            bins[...] += lax.dot_general(left, there, NT, preferred_element_type=F32)
            return carry

        lax.fori_loop(0, target.shape[0] // (4 * each), body, 0, unroll=2)
        planes = (
            bins[:rows] + bins[rows : 2 * rows],
            bins[2 * rows : 3 * rows] * 256.0 + bins[3 * rows :],
        )
        if 2 * rows_a_plane < SUBLANES:
            send[...] = jnp.zeros_like(send)
        for i, plane in enumerate(planes):
            for row in range(rows_a_plane):
                first, col = divmod(row * LANES, lane_count)
                send[pl.ds(i * rows_a_plane + row, devices, stride=SUBLANES), :] = plane[
                    first * devices : (first + 1) * devices, col : col + LANES
                ]

    def bin_copy(j):
        to_x, to_y = peer(j)
        at = pl.multiple_of((to_x * ny + to_y) * SUBLANES, SUBLANES)
        return pltpu.make_async_remote_copy(
            send.at[pl.ds(at, SUBLANES)], land.at[j], asend.at[0], arecv.at[j // together],
            device_id={"gx": to_x, "gy": to_y}, device_id_type=MESH,
        )

    def inject(step, sources):
        def one(j):
            amp = wide(land.at[j], 0, rows_a_plane)
            code = wide(land.at[j], rows_a_plane, rows_a_plane).astype(jnp.int32)
            cell, kind = parted(code, kind_count)
            upper, lower = parted(cell, low_count)
            picked = jnp.dot(table[step], picks(kind, kind_count), preferred_element_type=F32)
            currents = ((picked[:size] + picked[size:]) * amp).astype(BF16)
            high = packed_row(upper, size)
            left = [jnp.where(high == BF16(h), currents, BF16(0)) for h in range(high_count)]
            return jnp.concatenate(left, axis=0), picks(lower, low_count)

        left, hits = (jnp.concatenate(x, axis=1) for x in zip(*[one(j) for j in sources]))
        inj[step] += lax.dot_general(left, hits, NT, preferred_element_type=F32)

    def injected(step, c):
        h, col = divmod(c * LANES, low_count)
        return inj[step, h * size : (h + 1) * size, col : col + LANES]

    def inject_part(step, part, parts):
        each = devices // parts

        def body(q, carry):
            inject(step, [part * each + q * together + i for i in range(together)])
            return carry

        lax.fori_loop(0, each // together, body, 0)

    inputs = [
        pltpu.make_async_copy(there, here, isem.at[i])
        for i, (there, here) in enumerate((
            (target_hbm, target), (cells_hbm, cells), (kinds_hbm, kinds), (amps_hbm, amps),
            (x_hbm, cond_x), (y_hbm, cond_y), (cap_hbm, cap), (via_hbm, via), (waves_hbm, waves),
        ))
    ]
    fetches = [
        pltpu.make_async_copy(v_hbm.at[:, c], v.at[c // tile_x, c % tile_x], vsem.at[0])
        for c in range(count)
    ]
    for copy in inputs[:4] + fetches + inputs[4:]:
        copy.start()
    for e in range(halos):
        for me, n, to in ((gx, nx, xl), (gy, ny, yl)):
            for side, last in ((0, 0), (1, n - 1)):
                @pl.when(me == last)
                def _():
                    to[e, side] = jnp.zeros(to.shape[2:], to.dtype)

    @pl.when(gx == 0)
    def _():
        xc[...] = jnp.zeros_like(xc)

    @pl.when(gy == 0)
    def _():
        yc[...] = jnp.zeros_like(yc)

    barrier = pltpu.get_barrier_semaphore()

    for j in range(1, devices):
        to_x, to_y = peer(j)
        pl.semaphore_signal(
            barrier, inc=1, device_id={"gx": to_x, "gy": to_y}, device_id_type=MESH
        )
    inputs[0].wait()
    find_spots()
    for copy in inputs[1:4]:
        copy.wait()
    fill_bins()
    settle(v, vsem.at[0])
    for copy in inputs[4:]:
        copy.wait()
    rim = Rim(0)
    for c in range(count):
        rim.add(c, v[c // tile_x, c % tile_x])
    pl.semaphore_wait(barrier, devices - 1)

    rims = rim_copies()
    pl.when(gx < nx - 1)(rims[0].start)
    pl.when(gy < ny - 1)(rims[1].start)

    for j in reversed(range(1, devices)):
        bin_copy(j).start()
    rim.send_x()
    rim.send_y()
    own = pl.multiple_of((gx * ny + gy) * SUBLANES, SUBLANES)
    land[0] = send[pl.ds(own, SUBLANES), :]
    wave_high, wave_low = halves(waves[...])
    for step in range(steps):
        at = slice(step * size, (step + 1) * size)
        table[step, :size] = wave_high[at]
        table[step, size:] = wave_low[at]
    inj[...] = jnp.zeros_like(inj)

    def first_inject(q, carry):
        @pl.when(q == 0)
        def _():
            settle(land.at[pl.ds(1, together - 1)], arecv.at[0])

        @pl.when(q > 0)
        def _():
            settle(land.at[pl.ds(q * together, together)], arecv.at[q])

        inject(0, [q * together + i for i in range(together)])
        return carry

    for i, (me, n) in enumerate(((gx, nx), (gy, ny))):
        pl.when(me > 0)(rims[i].wait_recv)
        pl.when(me < n - 1)(rims[i].wait_send)
    coefficients()
    inside(v, 1, k0)
    early = nx // together
    lax.fori_loop(0, early, first_inject, 0)
    arrive(0)
    rim = Rim(1)

    def first_residual(c, total):
        f = -SCALE * total
        k0[c // tile_x, c % tile_x] = f
        if c >= tile_x:
            split(0, c, f)
            rim.add(c, f)

    outside(k0, 0, first_residual, lambda: None)
    lax.fori_loop(early, devices // together, first_inject, 0)
    settle(send.at[pl.ds(0, (devices - 1) * SUBLANES)], asend.at[0])
    for c in range(tile_x):
        f = k0[0, c] - injected(0, c)
        k0[0, c] = f
        split(0, c, f)
        rim.add(c, f)
    rim.send_x()
    rim.send_y()

    def time_step(step, carry):
        e = 1 + ITERS * step
        more = step + 1 < steps

        def inject_next(part):
            @pl.when(more)
            def _():
                inject_part(step + 1, part, ITERS + 1)

        moments = grams([0], 0)
        inside(k0, 0, k1)
        inject_next(0)
        for j in range(1, ITERS + 1):
            arrive(e + j - 1)
            if j > 1:
                add_turn(step, j - 2)
            rim = Rim(e + j)

            def next_field(c, total):
                split(j, c, total)
                if j < ITERS:
                    fields[j][c // tile_x, c % tile_x] = total
                    rim.add(c, total)

            def send_edges():
                if j < ITERS:
                    rim.send_x()

            outside(fields[j], e + j - 1, next_field, send_edges)
            if j < ITERS:
                rim.send_y()
                moments = moments + grams([j - 1, j], j)
                inside(fields[j], 0, fields[j + 1])
                add_start(step, j - 1, moments)
                moments = []
            else:
                every_start(step, grams([j - 1], j)[0])
            inject_next(j)
        m = add_finish(step, 0) + add_finish(step, 1)
        m.append(jnp.zeros_like(m[0]))
        shifted_m = [SCALE * (m[i + 1] + SHIFT * m[i]) for i in range(len(m) - 1)]
        tiles = []
        for i in range(ITERS):
            for g in range(packed):
                tile = place(m[i], g, ITERS)
                for block in range(ITERS):
                    tile = jnp.where(group == block, place(shifted_m[i + block], g, block), tile)
                tiles.append(tile)
        early = (ITERS - 1) * packed
        for p in range(early):
            tiles = eliminate_panel(tiles, p)
        last = every_finish(step)
        for g in range(packed):
            at_end = jnp.where(group == ITERS - 1, SCALE * place(last, g, ITERS - 1), 0.0)
            tiles[early + g] = tiles[early + g] + at_end
        for p in range(early, ITERS * packed):
            tiles = eliminate_panel(tiles, p)
        solved = jnp.concatenate(tiles, axis=0)[:, ITERS * size : (ITERS + 1) * size]
        none = jnp.zeros((size, size), F32)
        take = jnp.concatenate([solved, none], axis=0)
        drop = jnp.concatenate([none, solved], axis=0)
        both = jnp.concatenate([take, -SCALE * (drop + SHIFT * take)], axis=1)
        high, low = halves(both)
        turned = jnp.concatenate([high.astype(F32), low.astype(F32)], axis=1).T.astype(BF16)
        turned = jnp.concatenate([turned, turned], axis=1)
        rim = Rim(jnp.minimum(e + ITERS, halos - 1))
        pairs = sorted({c - c % 2 for c in edges})
        for n, c in enumerate(pairs + [c for c in range(0, count, 2) if c not in pairs]):
            out = jnp.dot(
                turned, basis[:, c * LANES : (c + 2) * LANES], preferred_element_type=F32
            )
            out = out[: 2 * size] + out[2 * size :]
            for i in range(2):
                l, x = divmod(c + i, tile_x)
                cols = slice(i * LANES, (i + 1) * LANES)
                change = out[:size, cols]
                v[l, x] = v[l, x] + change
                left = k0[l, x] + out[size:, cols]
                r[l, x] = left
                left = left + k(9, c + i) * change
                if c + i < tile_x:
                    after = jnp.minimum(step + 1, steps - 1)
                    left = left - (injected(after, c + i) - injected(step, c + i))
                k0[l, x] = left
                split(0, c + i, left)
                rim.add(c + i, left)
            if n + 1 == len(pairs):
                pl.when(more)(rim.send_x)

        pl.when(more)(rim.send_y)
        return carry

    lax.fori_loop(0, steps, time_step, 0)
    for i, (here, there) in enumerate(((v, v_out), (r, r_out))):
        for c in range(count):
            pltpu.make_async_copy(
                here.at[c // tile_x, c % tile_x], there.at[:, c], osem.at[i]
            ).start()
    for i, here in enumerate((v, r)):
        settle(here, osem.at[i])


def hand_over_kernel(first, second, first_out, second_out, held, fetched, stored):
    pairs = ((first, first_out), (second, second_out))
    chunks = held.shape[1]
    each = first.shape[0] // chunks

    def fetch(i, n):
        return pltpu.make_async_copy(
            pairs[i][0].at[pl.ds(n * each, each)], held.at[i, n], fetched.at[i, n]
        )

    def store(i, n):
        return pltpu.make_async_copy(
            held.at[i, n], pairs[i][1].at[pl.ds(n * each, each)], stored.at[i, n]
        )

    order = [(i, n) for n in range(chunks) for i in range(2)]
    for where in order:
        fetch(*where).start()
    for where in order:
        fetch(*where).wait()
        store(*where).start()
    for where in order:
        store(*where).wait()


def hand_over(first, second):
    chunks = 4
    dma = pltpu.SemaphoreType.DMA
    return pl.pallas_call(
        hand_over_kernel,
        out_shape=[jax.ShapeDtypeStruct(first.shape, F32)] * 2,
        in_specs=[pl.BlockSpec(memory_space=pltpu.HBM)] * 2,
        out_specs=[pl.BlockSpec(memory_space=pltpu.HBM)] * 2,
        scratch_shapes=[
            pltpu.VMEM((2, chunks, first.shape[0] // chunks) + first.shape[1:], F32),
            dma((2, chunks)), dma((2, chunks)),
        ],
        compiler_params=pltpu.CompilerParams(vmem_limit_bytes=67043328),
        name="hand_over",
    )(first, second)


def body(volts, cap, cond_x, cond_y, via, waveforms, placement, cells, wave_ids, amps):
    nx, ny = lax.axis_size("gx"), lax.axis_size("gy")
    devices = nx * ny
    size, layers, tile_x, tile_y = volts.shape
    steps = waveforms.shape[0] // size
    count = layers * tile_x
    capacity = 2 * cells.shape[0] // devices
    lane_count = min(capacity, 2 * LANES)
    halos = 1 + steps * ITERS
    packed = (2 * ITERS - 1) * size * size // LANES
    low_count = 2 * LANES
    high_count = tile_x * tile_y // low_count
    field = (layers, tile_x, size, LANES)
    dma = pltpu.SemaphoreType.DMA
    flat = (count, tile_y)
    many = (cells.shape[0] // LANES, LANES)
    out, residual = pl.pallas_call(
        functools.partial(grid_kernel, nx, ny, steps, layers, tile_x, capacity),
        out_shape=[jax.ShapeDtypeStruct((size, count, LANES), F32)] * 2,
        in_specs=[pl.BlockSpec(memory_space=pltpu.HBM)] * 10,
        out_specs=[pl.BlockSpec(memory_space=pltpu.HBM)] * 2,
        scratch_shapes=[
            pltpu.VMEM(field, F32),
            pltpu.VMEM(field, F32),
            *[pltpu.VMEM(flat, F32)] * 4,
            pltpu.VMEM(waveforms.shape, F32),
            *[pltpu.VMEM(many, jnp.int32)] * 3,
            pltpu.VMEM(many, F32),
            dma((9,)), dma((1,)), dma((2,)),
            pltpu.VMEM(field, F32),
            pltpu.VMEM(field, F32),
            pltpu.VMEM(field, F32),
            pltpu.VMEM(field, F32),
            pltpu.VMEM((2 * (ITERS + 1) * size, count * LANES), BF16),
            pltpu.VMEM((halos, 2, layers, size, LANES), BF16),
            pltpu.VMEM((halos, 2, layers, size, LANES), BF16),
            pltpu.VMEM((halos, size, LANES), F32),
            pltpu.VMEM((halos, 2, size, LANES), F32),
            pltpu.VMEM((steps, nx, packed, LANES), F32),
            pltpu.VMEM((steps, ny, packed, LANES), F32),
            pltpu.VMEM((steps, devices, size * size // LANES, LANES), F32),
            pltpu.VMEM((10,) + flat, F32),
            pltpu.VMEM(flat, F32),
            pltpu.VMEM(flat, F32),
            pltpu.VMEM(many, jnp.int32),
            pltpu.VMEM((4 * devices * capacity // lane_count, lane_count), F32),
            pltpu.VMEM((devices * SUBLANES, LANES), F32),
            pltpu.VMEM((devices, SUBLANES, LANES), F32),
            pltpu.VMEM((steps, 2 * size, waveforms.shape[1]), BF16),
            pltpu.VMEM((steps, high_count * size, low_count), F32),
            *[dma((2, 2))] * 4,
            *[dma((steps, ITERS - 1))] * 4,
            dma((2,)), dma((2,)), dma((1,)), dma((devices // 4,)),
            dma((steps,)), dma((steps,)),
        ],
        compiler_params=pltpu.CompilerParams(
            collective_id=0, has_side_effects=True, vmem_limit_bytes=67043328
        ),
        name="transient",
    )(
        volts.reshape(size, count, tile_y),
        *[x.reshape(flat) for x in (cap, cond_x, cond_y, via)],
        waveforms,
        *[x.reshape(many) for x in (placement, cells, wave_ids, amps)],
    )
    out, residual = hand_over(out, residual)
    return out.reshape(volts.shape), residual.reshape(volts.shape)


def solution(mesh):
    grid = P(None, "gx", "gy")
    field = P(None, None, "gx", "gy")
    flat = P(("gx", "gy"))
    return jax.shard_map(
        body,
        mesh=mesh,
        in_specs=(field, grid, grid, grid, grid, P(), P(("gx", "gy"), None), flat, flat, flat),
        out_specs=(field, field),
        check_vma=False,
    )
```

```python
import functools

import jax
import jax.numpy as jnp
from jax import lax
from jax.experimental import pallas as pl
from jax.experimental.pallas import tpu as pltpu
from jax.sharding import PartitionSpec as P

ITERS = 3
SUBLANES = 8
SCALE = 6.0
SHIFT = 1.125
LANES = 128
MESH = pl.DeviceIdType.MESH
NT = (((1,), (1,)), ((), ()))
F32 = jnp.float32
BF16 = jnp.bfloat16


def rows_iota(rows, cols):
    return lax.broadcasted_iota(jnp.int32, (rows, cols), 0)


def ones(mask):
    return mask.astype(F32).astype(BF16)


def picks(row, count):
    lines = rows_iota(count, row.shape[1]).astype(F32).astype(BF16)
    return jnp.where(lines == packed_row(row, count), BF16(1), BF16(0))


def packed_row(row, count):
    once = jnp.broadcast_to(row.astype(F32), (2 * SUBLANES, row.shape[1])).astype(BF16)
    return jnp.concatenate([once] * (count // (2 * SUBLANES)), axis=0)


def parted(x, count):
    return x >> (count.bit_length() - 1), x & (count - 1)


def wide(ref, row, count):
    return jnp.concatenate([ref[pl.ds(row + i, 1), :] for i in range(count)], axis=1)


def across(tile, k):
    return jnp.broadcast_to(tile[:, k : k + 1], tile.shape)


def down(tile, a):
    return jnp.broadcast_to(tile[a : a + 1, :], tile.shape)


def eliminate_panel(tiles, p):
    tile, k = tiles[p], SUBLANES * p
    sub = rows_iota(SUBLANES, LANES)
    columns = [across(tile, k + b) for b in range(SUBLANES)]
    pivot = [[down(columns[b], a) for b in range(SUBLANES)] for a in range(SUBLANES)]
    right = [down(tile, a) for a in range(SUBLANES)]
    inverse = []
    for a in range(SUBLANES):
        inverse.append(1.0 / pivot[a][a])
        for b in range(a + 1, SUBLANES):
            factor = pivot[a][b] * inverse[a]
            right[b] = right[b] - factor * right[a]
            for c in range(b, SUBLANES):
                pivot[b][c] = pivot[b][c] - factor * pivot[a][c]
    solved = [None] * SUBLANES
    for a in reversed(range(SUBLANES)):
        row = right[a]
        for b in reversed(range(a + 1, SUBLANES)):
            row = row - pivot[a][b] * solved[b]
        solved[a] = row * inverse[a]
    fresh = []
    for i, other in enumerate(tiles):
        if i == p:
            result = solved[0]
            for a in range(1, SUBLANES):
                result = jnp.where(sub == a, solved[a], result)
        else:
            result = other
            for b in range(SUBLANES):
                result = result - across(other, k + b) * solved[b]
        fresh.append(result)
    return fresh


def halves(x):
    high = x.astype(BF16)
    return high, (x - high.astype(F32)).astype(BF16)


def settle(ref, semaphore):
    pltpu.make_async_copy(ref, ref, semaphore).wait()


def grid_kernel(
    nx, ny, steps, layers, tile_x, capacity,
    v_hbm, cap_hbm, x_hbm, y_hbm, via_hbm, waves_hbm, target_hbm, cells_hbm, kinds_hbm, amps_hbm,
    v_out, r_out,
    v, r, cap, cond_x, cond_y, via, waves, target, cells, kinds, amps, isem, vsem, osem,
    k0, k1, k2, k3, basis, xs, xl, ys, yl, gl, hl, al,
    coef, strip, xc, yc, spots, bins, send, land, table, inj,
    xsend, xrecv, ysend, yrecv, gsend, grecv, hsend, hrecv, csend, crecv, asend, arecv, fsend, frecv,
):
    gx, gy = lax.axis_index("gx"), lax.axis_index("gy")
    size = xs.shape[3]
    count = layers * tile_x
    halos = 1 + ITERS * steps
    packed = LANES // size
    part = size // packed
    spans = ((0, 3 * part), (3 * part, 2 * part))
    lane = lax.broadcasted_iota(jnp.int32, (size, LANES), 1)
    group = lax.broadcasted_iota(jnp.int32, (part, LANES), 1) // size
    edges = [l * tile_x + x for l in range(layers) for x in (0, tile_x - 1)]
    inner = [c for c in range(count) if c not in edges]
    fields = (k0, k1, k2, k3)
    devices = nx * ny
    low_count = inj.shape[2]
    high_count = inj.shape[1] // size
    kind_count = waves.shape[1]
    lane_count = bins.shape[1]
    rows_a_plane = capacity // LANES
    together = 4

    def walk(me, n):
        flips = [2**b * (1 - 2 * ((me // 2**b) % 2)) for b in range(n.bit_length() - 1)]
        places = [me]
        for flip in flips:
            places += [place + flip for place in places]
        return places

    walk_x, walk_y = walk(gx, nx), walk(gy, ny)

    def peer(j):
        return walk_x[j % nx], walk_y[j // nx]

    def x_copies(e):
        return [
            pltpu.make_async_remote_copy(
                xs.at[e, side], xl.at[e, side], xsend.at[e % 2, side], xrecv.at[e % 2, side],
                device_id={"gx": gx + (1 if side == 0 else -1)}, device_id_type=MESH,
            )
            for side in range(2)
        ]

    def y_copies(e):
        return [
            pltpu.make_async_remote_copy(
                ys.at[e], yl.at[e, side], ysend.at[e % 2, side], yrecv.at[e % 2, side],
                device_id={"gy": gy + (1 if side == 0 else -1)},
                device_id_type=MESH,
            )
            for side in range(2)
        ]

    def start(copies, me, n):
        pl.when(me < n - 1)(copies[0].start)
        pl.when(me > 0)(copies[1].start)

    def finish(copies, me, n):
        @pl.when(me > 0)
        def _():
            copies[0].wait_recv()
            copies[1].wait_send()

        @pl.when(me < n - 1)
        def _():
            copies[1].wait_recv()
            copies[0].wait_send()

    def arrive(e):
        finish(x_copies(e), gx, nx)
        finish(y_copies(e), gy, ny)

    class Rim:
        def __init__(self, e):
            self.e = e
            self.both = jnp.zeros((size, LANES), F32)

        def add(self, c, f):
            l, x = divmod(c, tile_x)
            for side, edge in ((0, tile_x - 1), (1, 0)):
                if x == edge:
                    xs[self.e, side, l] = f.astype(BF16)
            self.both = jnp.where(lane // 2 == c, pltpu.roll(f, 2 * c + 1, 1), self.both)

        def send_x(self):
            start(x_copies(self.e), gx, nx)

        def send_y(self):
            ys[self.e] = self.both
            start(y_copies(self.e), gy, ny)

    def k(i, c):
        return coef[i, c : c + 1, :]

    def inside(src, own, dst):
        for c in range(count):
            l, x = divmod(c, tile_x)
            f = src[l, x]
            total = k(own, c) * f
            if x + 1 < tile_x:
                total = total - k(2, c) * src[l, x + 1]
            if x:
                total = total - k(3, c) * src[l, x - 1]
            total = total - k(4, c) * pltpu.roll(f, LANES - 1, 1) - k(5, c) * pltpu.roll(f, 1, 1)
            if l + 1 < layers:
                total = total - k(6, c) * src[l + 1, x]
            if l:
                total = total - k(7, c) * src[l - 1, x]
            dst[l, x] = total

    def outside(dst, e, emit, after_edges):
        rims = jnp.where(lane % 2 == 0, yl[e, 0], pltpu.roll(yl[e, 1], LANES - 2, 1))
        for n, c in enumerate(edges + inner):
            l, x = divmod(c, tile_x)
            moved = pltpu.roll(rims, LANES - 2 * c, 1) if c else rims
            total = dst[l, x] - k(8, c) * moved
            if x + 1 == tile_x:
                total = total - k(2, c) * xl[e, 1, l].astype(F32)
            if x == 0:
                total = total - k(3, c) * xl[e, 0, l].astype(F32)
            emit(c, total)
            if n + 1 == len(edges):
                after_edges()

    def split(j, c, f):
        high, low = halves(f)
        cols = slice(c * LANES, (c + 1) * LANES)
        basis[j * size : (j + 1) * size, cols] = high
        basis[(ITERS + 1 + j) * size : (ITERS + 2 + j) * size, cols] = low

    def grams(left, j):
        def rows(i):
            return [basis[b * size : (b + 1) * size, :] for b in (i, ITERS + 1 + i)]

        every = [block for i in left for block in rows(i)]
        product = lax.dot_general(
            jnp.concatenate(every, axis=0), jnp.concatenate(rows(j), axis=0), NT,
            preferred_element_type=F32,
        )
        product = product[:, :size] + product[:, size:]
        return [
            product[2 * i * size : (2 * i + 1) * size] + product[(2 * i + 1) * size : (2 * i + 2) * size]
            for i in range(len(left))
        ]

    def rim_gram(e):
        beyond = jnp.where(
            lane % 2 == 0, pltpu.roll(yl[e, 1], LANES - 1, 1), pltpu.roll(yl[e, 0], 1, 1)
        )
        left, right = [halves(ys[e])], [halves(-(strip[:1] * beyond))]
        for c in edges:
            l, x = divmod(c, tile_x)
            side, i = (1, 2) if x else (0, 3)
            cols = slice(c * LANES, (c + 1) * LANES)
            left.append([
                basis[b * size : (b + 1) * size, cols] for b in (ITERS - 1, 2 * ITERS)
            ])
            right.append(halves(-(k(i, c) * xl[e, side, l].astype(F32))))
        left, right = (
            jnp.concatenate([jnp.concatenate(part, axis=0) for part in parts], axis=1)
            for parts in (left, right)
        )
        product = lax.dot_general(left, right, NT, preferred_element_type=F32)
        product = product[:, :size] + product[:, size:]
        return product[:size] + product[size:]

    def pack(matrix):
        return jnp.concatenate([matrix[i * part : (i + 1) * part] for i in range(packed)], axis=1)

    def gather(land, step, g, ssem, rsem, axis, places):
        rows = pl.ds(spans[g][0], spans[g][1])
        return [
            pltpu.make_async_remote_copy(
                land.at[step, places[0], rows], land.at[step, places[0], rows],
                ssem.at[step, g], rsem.at[step, g],
                device_id={axis: places[j]}, device_id_type=MESH,
            )
            for j in range(1, len(places))
        ]

    def along_x(step, g):
        return gather(gl, step, g, gsend, grecv, "gx", walk_x)

    def along_y(step, g):
        return gather(hl, step, g, hsend, hrecv, "gy", walk_y)

    def add_start(step, g, matrices):
        for i, matrix in enumerate(matrices):
            gl[step, gx, pl.ds(spans[g][0] + i * part, part), :] = pack(matrix)
        for copy in along_x(step, g):
            copy.start()

    def landed(land, ssem, rsem, step, g, n):
        first, rows = spans[g]
        for semaphore in (ssem, rsem):
            settle(land.at[step, pl.ds(0, n - 1), pl.ds(first, rows)], semaphore.at[step, g])
        total = land[step, 0, first : first + rows, :]
        for j in range(1, n):
            total = total + land[step, j, first : first + rows, :]
        return total

    def add_turn(step, g):
        total = landed(gl, gsend, grecv, step, g, nx)
        hl[step, gy, pl.ds(*spans[g]), :] = total
        for copy in along_y(step, g):
            copy.start()

    def add_finish(step, g):
        total = landed(hl, hsend, hrecv, step, g, ny)
        return [total[i * part : (i + 1) * part] for i in range(spans[g][1] // part)]

    def every_copy(step, j):
        to_x, to_y = peer(j)
        me = gx * ny + gy
        return pltpu.make_async_remote_copy(
            al.at[step, me], al.at[step, me], fsend.at[step], frecv.at[step],
            device_id={"gx": to_x, "gy": to_y}, device_id_type=MESH,
        )

    def every_start(step, matrix):
        al[step, gx * ny + gy] = pack(matrix)
        for j in reversed(range(1, devices)):
            every_copy(step, j).start()

    def every_finish(step):
        for semaphore in (fsend, frecv):
            settle(al.at[step, pl.ds(0, devices - 1)], semaphore.at[step])
        terms = [al[step, j] for j in range(devices)]
        while len(terms) > 1:
            terms = [a + b for a, b in zip(terms[::2], terms[1::2])]
        return terms[0]

    def place(matrix, g, block):
        shift = ((block - g) * size) % LANES
        return pltpu.roll(matrix, shift, 1) if shift else matrix

    def rim_copies():
        return [
            pltpu.make_async_remote_copy(
                from_ref, to_ref, csend.at[i], crecv.at[i],
                device_id={axis: me + 1}, device_id_type=MESH,
            )
            for i, (from_ref, to_ref, axis, me, n) in enumerate(
                ((cond_x, xc, "gx", gx, nx), (cond_y, yc, "gy", gy, ny))
            )
        ]

    def coefficients():
        row = rows_iota(tile_x, LANES)
        col = lax.broadcasted_iota(jnp.int32, (tile_x, LANES), 1)
        above = jnp.zeros((tile_x, LANES), F32)
        for l in range(layers):
            at = slice(l * tile_x, (l + 1) * tile_x)
            x_low = jnp.where(row == 0, pltpu.roll(xc[at], 1, 0), pltpu.roll(cond_x[at], 1, 0))
            y_low = jnp.where(col == 0, pltpu.roll(yc[at], 1, 1), pltpu.roll(cond_y[at], 1, 1))
            x_end = jnp.logical_and(row == tile_x - 1, gx == nx - 1)
            y_end = jnp.logical_and(col == LANES - 1, gy == ny - 1)
            around = cond_x[at] + x_low + cond_y[at] + y_low + via[at] + above
            first, final = col == 0, col == LANES - 1
            y_next = jnp.where(y_end, 0.0, cond_y[at])
            values = [
                (cap[at] + around) / SCALE - SHIFT, around / SCALE,
                jnp.where(x_end, 0.0, cond_x[at]) / SCALE, x_low / SCALE,
                jnp.where(final, 0.0, y_next) / SCALE, jnp.where(first, 0.0, y_low) / SCALE,
                via[at] / SCALE, above / SCALE,
                jnp.where(final, y_next, jnp.where(first, y_low, 0.0)) / SCALE, cap[at],
            ]
            for i, value in enumerate(values):
                coef[i, at] = value
            above = via[at]
        ends = jnp.zeros((1, LANES), F32)
        for c in range(count):
            ends = jnp.where(lane[:1] // 2 == c, pltpu.roll(k(8, c), 2 * c + 1, 1), ends)
        strip[:1] = ends

    def find_spots():
        width = 2 * LANES
        before = ones(rows_iota(width, width) < lax.broadcasted_iota(jnp.int32, (width, width), 1))
        together = 8

        def body(q, base):
            hits = [
                (rows_iota(devices, width) == wide(target, (q * together + i) * 2, 2)).astype(F32)
                for i in range(together)
            ]
            ahead = jnp.dot(
                jnp.concatenate(hits, axis=0).astype(BF16), before, preferred_element_type=F32
            )
            for i, hit in enumerate(hits):
                count = ahead[i * devices : (i + 1) * devices]
                spot = jnp.sum(hit * (count + base), axis=0, keepdims=True).astype(jnp.int32)
                for half in range(2):
                    at = pl.ds((q * together + i) * 2 + half, 1)
                    spots[at, :] = spot[:, half * LANES : (half + 1) * LANES]
                base = base + jnp.broadcast_to((count + hit)[:, width - 1 :], base.shape)
            return base

        lax.fori_loop(
            0, target.shape[0] // (2 * together), body, jnp.zeros((devices, width), F32)
        )

    def fill_bins():
        rows = bins.shape[0] // 4
        width = 4 * LANES
        each = 2
        bins[...] = jnp.zeros_like(bins)

        def one(b):
            upper, lower = parted(wide(spots, b * 4, 4), lane_count)
            key = wide(target, b * 4, 4) + upper * devices
            hits = rows_iota(rows, width).astype(F32).astype(BF16) == packed_row(key, rows)
            code = wide(cells, b * 4, 4) * kind_count + wide(kinds, b * 4, 4)
            amp = wide(amps, b * 4, 4)
            amp_high = amp.astype(BF16).astype(F32)
            parts = (amp_high, amp - amp_high, code >> 8, code & 255)
            left = [jnp.where(hits, packed_row(p, rows), BF16(0)) for p in parts]
            return jnp.concatenate(left, axis=0), picks(lower, lane_count)

        def body(b, carry):
            pairs = [one(b * each + i) for i in range(each)]
            left, there = (jnp.concatenate(x, axis=1) for x in zip(*pairs))
            bins[...] += lax.dot_general(left, there, NT, preferred_element_type=F32)
            return carry

        lax.fori_loop(0, target.shape[0] // (4 * each), body, 0, unroll=2)
        planes = (
            bins[:rows] + bins[rows : 2 * rows],
            bins[2 * rows : 3 * rows] * 256.0 + bins[3 * rows :],
        )
        if 2 * rows_a_plane < SUBLANES:
            send[...] = jnp.zeros_like(send)
        for i, plane in enumerate(planes):
            for row in range(rows_a_plane):
                first, col = divmod(row * LANES, lane_count)
                send[pl.ds(i * rows_a_plane + row, devices, stride=SUBLANES), :] = plane[
                    first * devices : (first + 1) * devices, col : col + LANES
                ]

    def bin_copy(j):
        to_x, to_y = peer(j)
        at = pl.multiple_of((to_x * ny + to_y) * SUBLANES, SUBLANES)
        return pltpu.make_async_remote_copy(
            send.at[pl.ds(at, SUBLANES)], land.at[j], asend.at[0], arecv.at[j // together],
            device_id={"gx": to_x, "gy": to_y}, device_id_type=MESH,
        )

    def inject(step, sources):
        def one(j):
            amp = wide(land.at[j], 0, rows_a_plane)
            code = wide(land.at[j], rows_a_plane, rows_a_plane).astype(jnp.int32)
            cell, kind = parted(code, kind_count)
            upper, lower = parted(cell, low_count)
            picked = jnp.dot(table[step], picks(kind, kind_count), preferred_element_type=F32)
            currents = ((picked[:size] + picked[size:]) * amp).astype(BF16)
            high = packed_row(upper, size)
            left = [jnp.where(high == BF16(h), currents, BF16(0)) for h in range(high_count)]
            return jnp.concatenate(left, axis=0), picks(lower, low_count)

        left, hits = (jnp.concatenate(x, axis=1) for x in zip(*[one(j) for j in sources]))
        inj[step] += lax.dot_general(left, hits, NT, preferred_element_type=F32)

    def injected(step, c):
        h, col = divmod(c * LANES, low_count)
        return inj[step, h * size : (h + 1) * size, col : col + LANES]

    def inject_part(step, part, parts):
        each = devices // parts

        def body(q, carry):
            inject(step, [part * each + q * together + i for i in range(together)])
            return carry

        lax.fori_loop(0, each // together, body, 0)

    inputs = [
        pltpu.make_async_copy(there, here, isem.at[i])
        for i, (there, here) in enumerate((
            (target_hbm, target), (cells_hbm, cells), (kinds_hbm, kinds), (amps_hbm, amps),
            (x_hbm, cond_x), (y_hbm, cond_y), (cap_hbm, cap), (via_hbm, via), (waves_hbm, waves),
        ))
    ]
    fetches = [
        pltpu.make_async_copy(v_hbm.at[:, c], v.at[c // tile_x, c % tile_x], vsem.at[0])
        for c in range(count)
    ]
    for copy in inputs[:4] + fetches + inputs[4:]:
        copy.start()
    for e in range(halos):
        for me, n, to in ((gx, nx, xl), (gy, ny, yl)):
            for side, last in ((0, 0), (1, n - 1)):
                @pl.when(me == last)
                def _():
                    to[e, side] = jnp.zeros(to.shape[2:], to.dtype)

    @pl.when(gx == 0)
    def _():
        xc[...] = jnp.zeros_like(xc)

    @pl.when(gy == 0)
    def _():
        yc[...] = jnp.zeros_like(yc)

    barrier = pltpu.get_barrier_semaphore()

    for j in range(1, devices):
        to_x, to_y = peer(j)
        pl.semaphore_signal(
            barrier, inc=1, device_id={"gx": to_x, "gy": to_y}, device_id_type=MESH
        )
    inputs[0].wait()
    find_spots()
    for copy in inputs[1:4]:
        copy.wait()
    fill_bins()
    settle(v, vsem.at[0])
    for copy in inputs[4:]:
        copy.wait()
    rim = Rim(0)
    for c in range(count):
        rim.add(c, v[c // tile_x, c % tile_x])
    pl.semaphore_wait(barrier, devices - 1)

    rims = rim_copies()
    pl.when(gx < nx - 1)(rims[0].start)
    pl.when(gy < ny - 1)(rims[1].start)

    for j in reversed(range(1, devices)):
        bin_copy(j).start()
    rim.send_x()
    rim.send_y()
    own = pl.multiple_of((gx * ny + gy) * SUBLANES, SUBLANES)
    land[0] = send[pl.ds(own, SUBLANES), :]
    wave_high, wave_low = halves(waves[...])
    for step in range(steps):
        at = slice(step * size, (step + 1) * size)
        table[step, :size] = wave_high[at]
        table[step, size:] = wave_low[at]
    inj[...] = jnp.zeros_like(inj)

    def first_inject(q, carry):
        @pl.when(q == 0)
        def _():
            settle(land.at[pl.ds(1, together - 1)], arecv.at[0])

        @pl.when(q > 0)
        def _():
            settle(land.at[pl.ds(q * together, together)], arecv.at[q])

        inject(0, [q * together + i for i in range(together)])
        return carry

    for i, (me, n) in enumerate(((gx, nx), (gy, ny))):
        pl.when(me > 0)(rims[i].wait_recv)
        pl.when(me < n - 1)(rims[i].wait_send)
    coefficients()
    inside(v, 1, k0)
    early = nx // together
    lax.fori_loop(0, early, first_inject, 0)
    arrive(0)
    rim = Rim(1)

    def first_residual(c, total):
        f = -SCALE * total
        k0[c // tile_x, c % tile_x] = f
        if c >= tile_x:
            split(0, c, f)
            rim.add(c, f)

    outside(k0, 0, first_residual, lambda: None)
    lax.fori_loop(early, devices // together, first_inject, 0)
    settle(send.at[pl.ds(0, (devices - 1) * SUBLANES)], asend.at[0])
    for c in range(tile_x):
        f = k0[0, c] - injected(0, c)
        k0[0, c] = f
        split(0, c, f)
        rim.add(c, f)
    rim.send_x()
    rim.send_y()

    def time_step(step, carry):
        e = 1 + ITERS * step
        more = step + 1 < steps

        def inject_next(part):
            @pl.when(more)
            def _():
                inject_part(step + 1, part, ITERS + 1)

        moments = grams([0], 0)
        inside(k0, 0, k1)
        inject_next(0)
        for j in range(1, ITERS + 1):
            arrive(e + j - 1)
            if j == ITERS:
                every_start(step, near + rim_gram(e + j - 1))
                add_turn(step, j - 2)
            rim = Rim(e + j)

            def next_field(c, total):
                split(j, c, total)
                if j < ITERS:
                    fields[j][c // tile_x, c % tile_x] = total
                    rim.add(c, total)

            def send_edges():
                if j < ITERS:
                    rim.send_x()

            outside(fields[j], e + j - 1, next_field, send_edges)
            if j < ITERS:
                rim.send_y()
                moments = moments + grams([j - 1, j], j)
                add_start(step, j - 1, moments)
                if j > 1:
                    add_turn(step, j - 2)
                inside(fields[j], 0, fields[j + 1])
                moments = []
            if j == ITERS - 1:
                for c in range(count):
                    split(ITERS, c, k3[c // tile_x, c % tile_x])
                (near,) = grams([j], ITERS)
            inject_next(j)
        m = add_finish(step, 0) + add_finish(step, 1)
        m.append(jnp.zeros_like(m[0]))
        shifted_m = [SCALE * (m[i + 1] + SHIFT * m[i]) for i in range(len(m) - 1)]
        tiles = []
        for i in range(ITERS):
            for g in range(packed):
                tile = place(m[i], g, ITERS)
                for block in range(ITERS):
                    tile = jnp.where(group == block, place(shifted_m[i + block], g, block), tile)
                tiles.append(tile)
        early = (ITERS - 1) * packed
        for p in range(early):
            tiles = eliminate_panel(tiles, p)
        last = every_finish(step)
        for g in range(packed):
            at_end = jnp.where(group == ITERS - 1, SCALE * place(last, g, ITERS - 1), 0.0)
            tiles[early + g] = tiles[early + g] + at_end
        for p in range(early, ITERS * packed):
            tiles = eliminate_panel(tiles, p)
        solved = jnp.concatenate(tiles, axis=0)[:, ITERS * size : (ITERS + 1) * size]
        none = jnp.zeros((size, size), F32)
        take = jnp.concatenate([solved, none], axis=0)
        drop = jnp.concatenate([none, solved], axis=0)
        both = jnp.concatenate([take, -SCALE * (drop + SHIFT * take)], axis=1)
        high, low = halves(both)
        turned = jnp.concatenate([high.astype(F32), low.astype(F32)], axis=1).T.astype(BF16)
        turned = jnp.concatenate([turned, turned], axis=1)
        rim = Rim(jnp.minimum(e + ITERS, halos - 1))
        pairs = sorted({c - c % 2 for c in edges})
        for n, c in enumerate(pairs + [c for c in range(0, count, 2) if c not in pairs]):
            out = jnp.dot(
                turned, basis[:, c * LANES : (c + 2) * LANES], preferred_element_type=F32
            )
            out = out[: 2 * size] + out[2 * size :]
            for i in range(2):
                l, x = divmod(c + i, tile_x)
                cols = slice(i * LANES, (i + 1) * LANES)
                change = out[:size, cols]
                v[l, x] = v[l, x] + change
                left = k0[l, x] + out[size:, cols]
                r[l, x] = left
                left = left + k(9, c + i) * change
                if c + i < tile_x:
                    after = jnp.minimum(step + 1, steps - 1)
                    left = left - (injected(after, c + i) - injected(step, c + i))
                k0[l, x] = left
                split(0, c + i, left)
                rim.add(c + i, left)
            if n + 1 == len(pairs):
                pl.when(more)(rim.send_x)

        pl.when(more)(rim.send_y)
        return carry

    lax.fori_loop(0, steps, time_step, 0)
    for i, (here, there) in enumerate(((v, v_out), (r, r_out))):
        for c in range(count):
            pltpu.make_async_copy(
                here.at[c // tile_x, c % tile_x], there.at[:, c], osem.at[i]
            ).start()
    for i, here in enumerate((v, r)):
        settle(here, osem.at[i])


def hand_over_kernel(first, second, first_out, second_out, held, fetched, stored):
    pairs = ((first, first_out), (second, second_out))
    chunks = held.shape[1]
    each = first.shape[0] // chunks

    def fetch(i, n):
        return pltpu.make_async_copy(
            pairs[i][0].at[pl.ds(n * each, each)], held.at[i, n], fetched.at[i, n]
        )

    def store(i, n):
        return pltpu.make_async_copy(
            held.at[i, n], pairs[i][1].at[pl.ds(n * each, each)], stored.at[i, n]
        )

    order = [(i, n) for n in range(chunks) for i in range(2)]
    for where in order:
        fetch(*where).start()
    for where in order:
        fetch(*where).wait()
        store(*where).start()
    for where in order:
        store(*where).wait()


def hand_over(first, second):
    chunks = 4
    dma = pltpu.SemaphoreType.DMA
    return pl.pallas_call(
        hand_over_kernel,
        out_shape=[jax.ShapeDtypeStruct(first.shape, F32)] * 2,
        in_specs=[pl.BlockSpec(memory_space=pltpu.HBM)] * 2,
        out_specs=[pl.BlockSpec(memory_space=pltpu.HBM)] * 2,
        scratch_shapes=[
            pltpu.VMEM((2, chunks, first.shape[0] // chunks) + first.shape[1:], F32),
            dma((2, chunks)), dma((2, chunks)),
        ],
        compiler_params=pltpu.CompilerParams(vmem_limit_bytes=67043328),
        name="hand_over",
    )(first, second)


def body(volts, cap, cond_x, cond_y, via, waveforms, placement, cells, wave_ids, amps):
    nx, ny = lax.axis_size("gx"), lax.axis_size("gy")
    devices = nx * ny
    size, layers, tile_x, tile_y = volts.shape
    steps = waveforms.shape[0] // size
    count = layers * tile_x
    capacity = 2 * cells.shape[0] // devices
    lane_count = min(capacity, 2 * LANES)
    halos = 1 + steps * ITERS
    packed = (2 * ITERS - 1) * size * size // LANES
    low_count = 2 * LANES
    high_count = tile_x * tile_y // low_count
    field = (layers, tile_x, size, LANES)
    dma = pltpu.SemaphoreType.DMA
    flat = (count, tile_y)
    many = (cells.shape[0] // LANES, LANES)
    out, residual = pl.pallas_call(
        functools.partial(grid_kernel, nx, ny, steps, layers, tile_x, capacity),
        out_shape=[jax.ShapeDtypeStruct((size, count, LANES), F32)] * 2,
        in_specs=[pl.BlockSpec(memory_space=pltpu.HBM)] * 10,
        out_specs=[pl.BlockSpec(memory_space=pltpu.HBM)] * 2,
        scratch_shapes=[
            pltpu.VMEM(field, F32),
            pltpu.VMEM(field, F32),
            *[pltpu.VMEM(flat, F32)] * 4,
            pltpu.VMEM(waveforms.shape, F32),
            *[pltpu.VMEM(many, jnp.int32)] * 3,
            pltpu.VMEM(many, F32),
            dma((9,)), dma((1,)), dma((2,)),
            pltpu.VMEM(field, F32),
            pltpu.VMEM(field, F32),
            pltpu.VMEM(field, F32),
            pltpu.VMEM(field, F32),
            pltpu.VMEM((2 * (ITERS + 1) * size, count * LANES), BF16),
            pltpu.VMEM((halos, 2, layers, size, LANES), BF16),
            pltpu.VMEM((halos, 2, layers, size, LANES), BF16),
            pltpu.VMEM((halos, size, LANES), F32),
            pltpu.VMEM((halos, 2, size, LANES), F32),
            pltpu.VMEM((steps, nx, packed, LANES), F32),
            pltpu.VMEM((steps, ny, packed, LANES), F32),
            pltpu.VMEM((steps, devices, size * size // LANES, LANES), F32),
            pltpu.VMEM((10,) + flat, F32),
            pltpu.VMEM((SUBLANES, LANES), F32),
            pltpu.VMEM(flat, F32),
            pltpu.VMEM(flat, F32),
            pltpu.VMEM(many, jnp.int32),
            pltpu.VMEM((4 * devices * capacity // lane_count, lane_count), F32),
            pltpu.VMEM((devices * SUBLANES, LANES), F32),
            pltpu.VMEM((devices, SUBLANES, LANES), F32),
            pltpu.VMEM((steps, 2 * size, waveforms.shape[1]), BF16),
            pltpu.VMEM((steps, high_count * size, low_count), F32),
            *[dma((2, 2))] * 4,
            *[dma((steps, ITERS - 1))] * 4,
            dma((2,)), dma((2,)), dma((1,)), dma((devices // 4,)),
            dma((steps,)), dma((steps,)),
        ],
        compiler_params=pltpu.CompilerParams(
            collective_id=0, has_side_effects=True, vmem_limit_bytes=67043328
        ),
        name="transient",
    )(
        volts.reshape(size, count, tile_y),
        *[x.reshape(flat) for x in (cap, cond_x, cond_y, via)],
        waveforms,
        *[x.reshape(many) for x in (placement, cells, wave_ids, amps)],
    )
    out, residual = hand_over(out, residual)
    return out.reshape(volts.shape), residual.reshape(volts.shape)


def solution(mesh):
    grid = P(None, "gx", "gy")
    field = P(None, None, "gx", "gy")
    flat = P(("gx", "gy"))
    return jax.shard_map(
        body,
        mesh=mesh,
        in_specs=(field, grid, grid, grid, grid, P(), P(("gx", "gy"), None), flat, flat, flat),
        out_specs=(field, field),
        check_vma=False,
    )
```

```python
import functools

import jax
import jax.numpy as jnp
from jax import lax
from jax.experimental import pallas as pl
from jax.experimental.pallas import tpu as pltpu
from jax.sharding import PartitionSpec as P

ITERS = 3
SUBLANES = 8
SCALE = 6.0
SHIFT = 1.125
LANES = 128
MESH = pl.DeviceIdType.MESH
NT = (((1,), (1,)), ((), ()))
F32 = jnp.float32
BF16 = jnp.bfloat16


def rows_iota(rows, cols):
    return lax.broadcasted_iota(jnp.int32, (rows, cols), 0)


def ones(mask):
    return mask.astype(F32).astype(BF16)


def picks(row, count):
    lines = rows_iota(count, row.shape[1]).astype(F32).astype(BF16)
    return jnp.where(lines == packed_row(row, count), BF16(1), BF16(0))


def packed_row(row, count):
    once = jnp.broadcast_to(row.astype(F32), (2 * SUBLANES, row.shape[1])).astype(BF16)
    return jnp.concatenate([once] * (count // (2 * SUBLANES)), axis=0)


def parted(x, count):
    return x >> (count.bit_length() - 1), x & (count - 1)


def wide(ref, row, count):
    return jnp.concatenate([ref[pl.ds(row + i, 1), :] for i in range(count)], axis=1)


def across(tile, k):
    return jnp.broadcast_to(tile[:, k : k + 1], tile.shape)


def down(tile, a):
    return jnp.broadcast_to(tile[a : a + 1, :], tile.shape)


def eliminate_panel(tiles, p):
    tile, k = tiles[p], SUBLANES * p
    sub = rows_iota(SUBLANES, LANES)
    columns = [across(tile, k + b) for b in range(SUBLANES)]
    pivot = [[down(columns[b], a) for b in range(SUBLANES)] for a in range(SUBLANES)]
    right = [down(tile, a) for a in range(SUBLANES)]
    inverse = []
    for a in range(SUBLANES):
        inverse.append(1.0 / pivot[a][a])
        for b in range(a + 1, SUBLANES):
            factor = pivot[a][b] * inverse[a]
            right[b] = right[b] - factor * right[a]
            for c in range(b, SUBLANES):
                pivot[b][c] = pivot[b][c] - factor * pivot[a][c]
    solved = [None] * SUBLANES
    for a in reversed(range(SUBLANES)):
        row = right[a]
        for b in reversed(range(a + 1, SUBLANES)):
            row = row - pivot[a][b] * solved[b]
        solved[a] = row * inverse[a]
    fresh = []
    for i, other in enumerate(tiles):
        if i == p:
            result = solved[0]
            for a in range(1, SUBLANES):
                result = jnp.where(sub == a, solved[a], result)
        else:
            result = other
            for b in range(SUBLANES):
                result = result - across(other, k + b) * solved[b]
        fresh.append(result)
    return fresh


def halves(x):
    high = x.astype(BF16)
    return high, (x - high.astype(F32)).astype(BF16)


def settle(ref, semaphore):
    pltpu.make_async_copy(ref, ref, semaphore).wait()


def grid_kernel(
    nx, ny, steps, layers, tile_x, capacity,
    v_hbm, cap_hbm, x_hbm, y_hbm, via_hbm, waves_hbm, target_hbm, cells_hbm, kinds_hbm, amps_hbm,
    v_out, r_out,
    v, r, cap, cond_x, cond_y, via, waves, target, cells, kinds, amps, isem, vsem, osem,
    k0, k1, k2, k3, basis, xs, xl, ys, yl, gl, hl, al,
    coef, strip, xc, yc, spots, bins, send, land, table, inj,
    xsend, xrecv, ysend, yrecv, gsend, grecv, hsend, hrecv, csend, crecv, asend, arecv, fsend, frecv,
):
    gx, gy = lax.axis_index("gx"), lax.axis_index("gy")
    size = xs.shape[3]
    count = layers * tile_x
    halos = 1 + ITERS * steps
    packed = LANES // size
    part = size // packed
    spans = ((0, 3 * part), (3 * part, 2 * part))
    lane = lax.broadcasted_iota(jnp.int32, (size, LANES), 1)
    group = lax.broadcasted_iota(jnp.int32, (part, LANES), 1) // size
    edges = [l * tile_x + x for l in range(layers) for x in (0, tile_x - 1)]
    inner = [c for c in range(count) if c not in edges]
    fields = (k0, k1, k2, k3)
    devices = nx * ny
    low_count = inj.shape[2]
    high_count = inj.shape[1] // size
    kind_count = waves.shape[1]
    lane_count = bins.shape[1]
    rows_a_plane = capacity // LANES
    together = 4

    def walk(me, n):
        flips = [2**b * (1 - 2 * ((me // 2**b) % 2)) for b in range(n.bit_length() - 1)]
        places = [me]
        for flip in flips:
            places += [place + flip for place in places]
        return places

    walk_x, walk_y = walk(gx, nx), walk(gy, ny)

    def peer(j):
        return walk_x[j % nx], walk_y[j // nx]

    def x_copies(e):
        return [
            pltpu.make_async_remote_copy(
                xs.at[e, side], xl.at[e, side], xsend.at[e % 2, side], xrecv.at[e % 2, side],
                device_id={"gx": gx + (1 if side == 0 else -1)}, device_id_type=MESH,
            )
            for side in range(2)
        ]

    def y_copies(e):
        return [
            pltpu.make_async_remote_copy(
                ys.at[e], yl.at[e, side], ysend.at[e % 2, side], yrecv.at[e % 2, side],
                device_id={"gy": gy + (1 if side == 0 else -1)},
                device_id_type=MESH,
            )
            for side in range(2)
        ]

    def start(copies, me, n):
        pl.when(me < n - 1)(copies[0].start)
        pl.when(me > 0)(copies[1].start)

    def finish(copies, me, n):
        @pl.when(me > 0)
        def _():
            copies[0].wait_recv()
            copies[1].wait_send()

        @pl.when(me < n - 1)
        def _():
            copies[1].wait_recv()
            copies[0].wait_send()

    def arrive(e):
        finish(x_copies(e), gx, nx)
        finish(y_copies(e), gy, ny)

    class Rim:
        def __init__(self, e):
            self.e = e
            self.both = jnp.zeros((size, LANES), F32)

        def add(self, c, f):
            l, x = divmod(c, tile_x)
            for side, edge in ((0, tile_x - 1), (1, 0)):
                if x == edge:
                    xs[self.e, side, l] = f.astype(BF16)
            self.both = jnp.where(lane // 2 == c, pltpu.roll(f, 2 * c + 1, 1), self.both)

        def send_x(self):
            start(x_copies(self.e), gx, nx)

        def send_y(self):
            ys[self.e] = self.both
            start(y_copies(self.e), gy, ny)

    def k(i, c):
        return coef[i, c : c + 1, :]

    def inside(src, own, dst):
        for c in range(count):
            l, x = divmod(c, tile_x)
            f = src[l, x]
            total = k(own, c) * f
            if x + 1 < tile_x:
                total = total - k(2, c) * src[l, x + 1]
            if x:
                total = total - k(3, c) * src[l, x - 1]
            total = total - k(4, c) * pltpu.roll(f, LANES - 1, 1) - k(5, c) * pltpu.roll(f, 1, 1)
            if l + 1 < layers:
                total = total - k(6, c) * src[l + 1, x]
            if l:
                total = total - k(7, c) * src[l - 1, x]
            dst[l, x] = total

    def outside(dst, e, emit, after_edges):
        rims = jnp.where(lane % 2 == 0, yl[e, 0], pltpu.roll(yl[e, 1], LANES - 2, 1))
        for n, c in enumerate(edges + inner):
            l, x = divmod(c, tile_x)
            moved = pltpu.roll(rims, LANES - 2 * c, 1) if c else rims
            total = dst[l, x] - k(8, c) * moved
            if x + 1 == tile_x:
                total = total - k(2, c) * xl[e, 1, l].astype(F32)
            if x == 0:
                total = total - k(3, c) * xl[e, 0, l].astype(F32)
            emit(c, total)
            if n + 1 == len(edges):
                after_edges()

    def split(j, c, f):
        high, low = halves(f)
        cols = slice(c * LANES, (c + 1) * LANES)
        basis[j * size : (j + 1) * size, cols] = high
        basis[(ITERS + 1 + j) * size : (ITERS + 2 + j) * size, cols] = low

    def grams(left, j):
        def rows(i):
            return [basis[b * size : (b + 1) * size, :] for b in (i, ITERS + 1 + i)]

        every = [block for i in left for block in rows(i)]
        product = lax.dot_general(
            jnp.concatenate(every, axis=0), jnp.concatenate(rows(j), axis=0), NT,
            preferred_element_type=F32,
        )
        product = product[:, :size] + product[:, size:]
        return [
            product[2 * i * size : (2 * i + 1) * size] + product[(2 * i + 1) * size : (2 * i + 2) * size]
            for i in range(len(left))
        ]

    def rim_gram(e):
        beyond = jnp.where(
            lane % 2 == 0, pltpu.roll(yl[e, 1], LANES - 1, 1), pltpu.roll(yl[e, 0], 1, 1)
        )
        left, right = [halves(ys[e])], [halves(-(strip[:1] * beyond))]
        for c in edges:
            l, x = divmod(c, tile_x)
            side, i = (1, 2) if x else (0, 3)
            cols = slice(c * LANES, (c + 1) * LANES)
            left.append([
                basis[b * size : (b + 1) * size, cols] for b in (ITERS - 1, 2 * ITERS)
            ])
            right.append(halves(-(k(i, c) * xl[e, side, l].astype(F32))))
        left, right = (
            jnp.concatenate([jnp.concatenate(part, axis=0) for part in parts], axis=1)
            for parts in (left, right)
        )
        product = lax.dot_general(left, right, NT, preferred_element_type=F32)
        product = product[:, :size] + product[:, size:]
        return product[:size] + product[size:]

    def pack(matrix):
        return jnp.concatenate([matrix[i * part : (i + 1) * part] for i in range(packed)], axis=1)

    def gather(land, step, g, ssem, rsem, axis, places):
        rows = pl.ds(spans[g][0], spans[g][1])
        return [
            pltpu.make_async_remote_copy(
                land.at[step, places[0], rows], land.at[step, places[0], rows],
                ssem.at[step, g], rsem.at[step, g],
                device_id={axis: places[j]}, device_id_type=MESH,
            )
            for j in range(1, len(places))
        ]

    def along_x(step, g):
        return gather(gl, step, g, gsend, grecv, "gx", walk_x)

    def along_y(step, g):
        return gather(hl, step, g, hsend, hrecv, "gy", walk_y)

    def add_start(step, g, matrices):
        for i, matrix in enumerate(matrices):
            gl[step, gx, pl.ds(spans[g][0] + i * part, part), :] = pack(matrix)
        for copy in along_x(step, g):
            copy.start()

    def landed(land, ssem, rsem, step, g, n):
        first, rows = spans[g]
        for semaphore in (ssem, rsem):
            settle(land.at[step, pl.ds(0, n - 1), pl.ds(first, rows)], semaphore.at[step, g])
        total = land[step, 0, first : first + rows, :]
        for j in range(1, n):
            total = total + land[step, j, first : first + rows, :]
        return total

    def add_turn(step, g):
        total = landed(gl, gsend, grecv, step, g, nx)
        hl[step, gy, pl.ds(*spans[g]), :] = total
        for copy in along_y(step, g):
            copy.start()

    def add_finish(step, g):
        total = landed(hl, hsend, hrecv, step, g, ny)
        return [total[i * part : (i + 1) * part] for i in range(spans[g][1] // part)]

    def every_copy(step, j):
        to_x, to_y = peer(j)
        me = gx * ny + gy
        return pltpu.make_async_remote_copy(
            al.at[step, me], al.at[step, me], fsend.at[step], frecv.at[step],
            device_id={"gx": to_x, "gy": to_y}, device_id_type=MESH,
        )

    def every_start(step, matrix):
        al[step, gx * ny + gy] = pack(matrix)
        for j in reversed(range(1, devices)):
            every_copy(step, j).start()

    def every_finish(step):
        for semaphore in (fsend, frecv):
            settle(al.at[step, pl.ds(0, devices - 1)], semaphore.at[step])
        terms = [al[step, j] for j in range(devices)]
        while len(terms) > 1:
            terms = [a + b for a, b in zip(terms[::2], terms[1::2])]
        return terms[0]

    def place(matrix, g, block):
        shift = ((block - g) * size) % LANES
        return pltpu.roll(matrix, shift, 1) if shift else matrix

    def rim_copies():
        return [
            pltpu.make_async_remote_copy(
                from_ref, to_ref, csend.at[i], crecv.at[i],
                device_id={axis: me + 1}, device_id_type=MESH,
            )
            for i, (from_ref, to_ref, axis, me, n) in enumerate(
                ((cond_x, xc, "gx", gx, nx), (cond_y, yc, "gy", gy, ny))
            )
        ]

    def coefficients():
        row = rows_iota(tile_x, LANES)
        col = lax.broadcasted_iota(jnp.int32, (tile_x, LANES), 1)
        above = jnp.zeros((tile_x, LANES), F32)
        for l in range(layers):
            at = slice(l * tile_x, (l + 1) * tile_x)
            x_low = jnp.where(row == 0, pltpu.roll(xc[at], 1, 0), pltpu.roll(cond_x[at], 1, 0))
            y_low = jnp.where(col == 0, pltpu.roll(yc[at], 1, 1), pltpu.roll(cond_y[at], 1, 1))
            x_end = jnp.logical_and(row == tile_x - 1, gx == nx - 1)
            y_end = jnp.logical_and(col == LANES - 1, gy == ny - 1)
            around = cond_x[at] + x_low + cond_y[at] + y_low + via[at] + above
            first, final = col == 0, col == LANES - 1
            y_next = jnp.where(y_end, 0.0, cond_y[at])
            values = [
                (cap[at] + around) / SCALE - SHIFT, around / SCALE,
                jnp.where(x_end, 0.0, cond_x[at]) / SCALE, x_low / SCALE,
                jnp.where(final, 0.0, y_next) / SCALE, jnp.where(first, 0.0, y_low) / SCALE,
                via[at] / SCALE, above / SCALE,
                jnp.where(final, y_next, jnp.where(first, y_low, 0.0)) / SCALE, cap[at],
            ]
            for i, value in enumerate(values):
                coef[i, at] = value
            above = via[at]
        ends = jnp.zeros((1, LANES), F32)
        for c in range(count):
            ends = jnp.where(lane[:1] // 2 == c, pltpu.roll(k(8, c), 2 * c + 1, 1), ends)
        strip[:1] = ends

    def find_spots():
        width = 2 * LANES
        before = ones(rows_iota(width, width) < lax.broadcasted_iota(jnp.int32, (width, width), 1))
        together = 8

        def body(q, base):
            hits = [
                (rows_iota(devices, width) == wide(target, (q * together + i) * 2, 2)).astype(F32)
                for i in range(together)
            ]
            ahead = jnp.dot(
                jnp.concatenate(hits, axis=0).astype(BF16), before, preferred_element_type=F32
            )
            for i, hit in enumerate(hits):
                count = ahead[i * devices : (i + 1) * devices]
                spot = jnp.sum(hit * (count + base), axis=0, keepdims=True).astype(jnp.int32)
                for half in range(2):
                    at = pl.ds((q * together + i) * 2 + half, 1)
                    spots[at, :] = spot[:, half * LANES : (half + 1) * LANES]
                base = base + jnp.broadcast_to((count + hit)[:, width - 1 :], base.shape)
            return base

        lax.fori_loop(
            0, target.shape[0] // (2 * together), body, jnp.zeros((devices, width), F32)
        )

    def fill_bins():
        rows = bins.shape[0] // 4
        width = 4 * LANES
        each = 2
        bins[...] = jnp.zeros_like(bins)

        def one(b):
            upper, lower = parted(wide(spots, b * 4, 4), lane_count)
            key = wide(target, b * 4, 4) + upper * devices
            hits = rows_iota(rows, width).astype(F32).astype(BF16) == packed_row(key, rows)
            code = wide(cells, b * 4, 4) * kind_count + wide(kinds, b * 4, 4)
            amp = wide(amps, b * 4, 4)
            amp_high = amp.astype(BF16).astype(F32)
            parts = (amp_high, amp - amp_high, code >> 8, code & 255)
            left = [jnp.where(hits, packed_row(p, rows), BF16(0)) for p in parts]
            return jnp.concatenate(left, axis=0), picks(lower, lane_count)

        def body(b, carry):
            pairs = [one(b * each + i) for i in range(each)]
            left, there = (jnp.concatenate(x, axis=1) for x in zip(*pairs))
            bins[...] += lax.dot_general(left, there, NT, preferred_element_type=F32)
            return carry

        lax.fori_loop(0, target.shape[0] // (4 * each), body, 0, unroll=2)
        planes = (
            bins[:rows] + bins[rows : 2 * rows],
            bins[2 * rows : 3 * rows] * 256.0 + bins[3 * rows :],
        )
        if 2 * rows_a_plane < SUBLANES:
            send[...] = jnp.zeros_like(send)
        for i, plane in enumerate(planes):
            for row in range(rows_a_plane):
                first, col = divmod(row * LANES, lane_count)
                send[pl.ds(i * rows_a_plane + row, devices, stride=SUBLANES), :] = plane[
                    first * devices : (first + 1) * devices, col : col + LANES
                ]

    def bin_copy(j):
        to_x, to_y = peer(j)
        at = pl.multiple_of((to_x * ny + to_y) * SUBLANES, SUBLANES)
        return pltpu.make_async_remote_copy(
            send.at[pl.ds(at, SUBLANES)], land.at[j], asend.at[0], arecv.at[j // together],
            device_id={"gx": to_x, "gy": to_y}, device_id_type=MESH,
        )

    def inject(step, sources):
        def one(j):
            amp = wide(land.at[j], 0, rows_a_plane)
            code = wide(land.at[j], rows_a_plane, rows_a_plane).astype(jnp.int32)
            cell, kind = parted(code, kind_count)
            upper, lower = parted(cell, low_count)
            picked = jnp.dot(table[step], picks(kind, kind_count), preferred_element_type=F32)
            currents = ((picked[:size] + picked[size:]) * amp).astype(BF16)
            high = packed_row(upper, size)
            left = [jnp.where(high == BF16(h), currents, BF16(0)) for h in range(high_count)]
            return jnp.concatenate(left, axis=0), picks(lower, low_count)

        left, hits = (jnp.concatenate(x, axis=1) for x in zip(*[one(j) for j in sources]))
        inj[step] += lax.dot_general(left, hits, NT, preferred_element_type=F32)

    def injected(step, c):
        h, col = divmod(c * LANES, low_count)
        return inj[step, h * size : (h + 1) * size, col : col + LANES]

    def inject_part(step, part, parts):
        each = devices // parts

        def body(q, carry):
            inject(step, [part * each + q * together + i for i in range(together)])
            return carry

        lax.fori_loop(0, each // together, body, 0)

    inputs = [
        pltpu.make_async_copy(there, here, isem.at[i])
        for i, (there, here) in enumerate((
            (target_hbm, target), (cells_hbm, cells), (kinds_hbm, kinds), (amps_hbm, amps),
            (x_hbm, cond_x), (y_hbm, cond_y), (cap_hbm, cap), (via_hbm, via), (waves_hbm, waves),
        ))
    ]
    fetches = [
        pltpu.make_async_copy(v_hbm.at[:, c], v.at[c // tile_x, c % tile_x], vsem.at[0])
        for c in range(count)
    ]
    inputs[0].start()
    barrier = pltpu.get_barrier_semaphore()

    for j in range(1, devices):
        to_x, to_y = peer(j)
        pl.semaphore_signal(
            barrier, inc=1, device_id={"gx": to_x, "gy": to_y}, device_id_type=MESH
        )
    for copy in inputs[1:4] + fetches + inputs[4:]:
        copy.start()
    for me, n, to in ((gx, nx, xl), (gy, ny, yl)):
        for side, last in ((0, 0), (1, n - 1)):
            @pl.when(me == last)
            def _():
                for e in range(halos):
                    to[e, side] = jnp.zeros(to.shape[2:], to.dtype)

    @pl.when(gx == 0)
    def _():
        xc[...] = jnp.zeros_like(xc)

    @pl.when(gy == 0)
    def _():
        yc[...] = jnp.zeros_like(yc)

    inputs[0].wait()
    find_spots()
    for copy in inputs[1:4]:
        copy.wait()
    fill_bins()
    settle(v, vsem.at[0])
    for copy in inputs[4:]:
        copy.wait()
    rim = Rim(0)
    for c in range(count):
        rim.add(c, v[c // tile_x, c % tile_x])
    pl.semaphore_wait(barrier, devices - 1)

    rims = rim_copies()
    pl.when(gx < nx - 1)(rims[0].start)
    pl.when(gy < ny - 1)(rims[1].start)

    for j in reversed(range(1, devices)):
        bin_copy(j).start()
    rim.send_x()
    rim.send_y()
    own = pl.multiple_of((gx * ny + gy) * SUBLANES, SUBLANES)
    land[0] = send[pl.ds(own, SUBLANES), :]
    wave_high, wave_low = halves(waves[...])
    for step in range(steps):
        at = slice(step * size, (step + 1) * size)
        table[step, :size] = wave_high[at]
        table[step, size:] = wave_low[at]
    inj[...] = jnp.zeros_like(inj)

    def first_inject(q, carry):
        @pl.when(q == 0)
        def _():
            settle(land.at[pl.ds(1, together - 1)], arecv.at[0])

        @pl.when(q > 0)
        def _():
            settle(land.at[pl.ds(q * together, together)], arecv.at[q])

        inject(0, [q * together + i for i in range(together)])
        return carry

    for i, (me, n) in enumerate(((gx, nx), (gy, ny))):
        pl.when(me > 0)(rims[i].wait_recv)
        pl.when(me < n - 1)(rims[i].wait_send)
    coefficients()
    inside(v, 1, k0)
    early = nx // together
    lax.fori_loop(0, early, first_inject, 0)
    arrive(0)
    rim = Rim(1)

    def first_residual(c, total):
        f = -SCALE * total
        k0[c // tile_x, c % tile_x] = f
        if c >= tile_x:
            split(0, c, f)
            rim.add(c, f)

    outside(k0, 0, first_residual, lambda: None)
    lax.fori_loop(early, devices // together, first_inject, 0)
    settle(send.at[pl.ds(0, (devices - 1) * SUBLANES)], asend.at[0])
    for c in range(tile_x):
        f = k0[0, c] - injected(0, c)
        k0[0, c] = f
        split(0, c, f)
        rim.add(c, f)
    rim.send_x()
    rim.send_y()

    def time_step(step, carry):
        e = 1 + ITERS * step
        more = step + 1 < steps

        def inject_next(part):
            @pl.when(more)
            def _():
                inject_part(step + 1, part, ITERS + 1)

        moments = grams([0], 0)
        inside(k0, 0, k1)
        inject_next(0)
        for j in range(1, ITERS + 1):
            arrive(e + j - 1)
            if j == ITERS:
                every_start(step, near + rim_gram(e + j - 1))
                add_turn(step, j - 2)
            rim = Rim(e + j)

            def next_field(c, total):
                split(j, c, total)
                if j < ITERS:
                    fields[j][c // tile_x, c % tile_x] = total
                    rim.add(c, total)

            def send_edges():
                if j < ITERS:
                    rim.send_x()

            outside(fields[j], e + j - 1, next_field, send_edges)
            if j < ITERS:
                rim.send_y()
                moments = moments + grams([j - 1, j], j)
                add_start(step, j - 1, moments)
                if j > 1:
                    add_turn(step, j - 2)
                inside(fields[j], 0, fields[j + 1])
                moments = []
            if j == ITERS - 1:
                for c in range(count):
                    split(ITERS, c, k3[c // tile_x, c % tile_x])
                (near,) = grams([j], ITERS)
            inject_next(j)
        m = add_finish(step, 0) + add_finish(step, 1)
        m.append(jnp.zeros_like(m[0]))
        shifted_m = [SCALE * (m[i + 1] + SHIFT * m[i]) for i in range(len(m) - 1)]
        tiles = []
        for i in range(ITERS):
            for g in range(packed):
                tile = place(m[i], g, ITERS)
                for block in range(ITERS):
                    tile = jnp.where(group == block, place(shifted_m[i + block], g, block), tile)
                tiles.append(tile)
        early = (ITERS - 1) * packed
        for p in range(early):
            tiles = eliminate_panel(tiles, p)
        last = every_finish(step)
        for g in range(packed):
            at_end = jnp.where(group == ITERS - 1, SCALE * place(last, g, ITERS - 1), 0.0)
            tiles[early + g] = tiles[early + g] + at_end
        for p in range(early, ITERS * packed):
            tiles = eliminate_panel(tiles, p)
        solved = jnp.concatenate(tiles, axis=0)[:, ITERS * size : (ITERS + 1) * size]
        none = jnp.zeros((size, size), F32)
        take = jnp.concatenate([solved, none], axis=0)
        drop = jnp.concatenate([none, solved], axis=0)
        both = jnp.concatenate([take, -SCALE * (drop + SHIFT * take)], axis=1)
        high, low = halves(both)
        turned = jnp.concatenate([high.astype(F32), low.astype(F32)], axis=1).T.astype(BF16)
        turned = jnp.concatenate([turned, turned], axis=1)
        rim = Rim(jnp.minimum(e + ITERS, halos - 1))
        pairs = sorted({c - c % 2 for c in edges})
        for n, c in enumerate(pairs + [c for c in range(0, count, 2) if c not in pairs]):
            out = jnp.dot(
                turned, basis[:, c * LANES : (c + 2) * LANES], preferred_element_type=F32
            )
            out = out[: 2 * size] + out[2 * size :]
            for i in range(2):
                l, x = divmod(c + i, tile_x)
                cols = slice(i * LANES, (i + 1) * LANES)
                change = out[:size, cols]
                v[l, x] = v[l, x] + change
                left = k0[l, x] + out[size:, cols]
                r[l, x] = left
                left = left + k(9, c + i) * change
                if c + i < tile_x:
                    after = jnp.minimum(step + 1, steps - 1)
                    left = left - (injected(after, c + i) - injected(step, c + i))
                k0[l, x] = left
                split(0, c + i, left)
                rim.add(c + i, left)
            if n + 1 == len(pairs):
                pl.when(more)(rim.send_x)

        pl.when(more)(rim.send_y)
        return carry

    lax.fori_loop(0, steps, time_step, 0)
    for i, (here, there) in enumerate(((v, v_out), (r, r_out))):
        for c in range(count):
            pltpu.make_async_copy(
                here.at[c // tile_x, c % tile_x], there.at[:, c], osem.at[i]
            ).start()
    for i, here in enumerate((v, r)):
        settle(here, osem.at[i])


def hand_over_kernel(first, second, first_out, second_out, held, fetched, stored):
    pairs = ((first, first_out), (second, second_out))
    chunks = held.shape[1]
    each = first.shape[0] // chunks

    def fetch(i, n):
        return pltpu.make_async_copy(
            pairs[i][0].at[pl.ds(n * each, each)], held.at[i, n], fetched.at[i, n]
        )

    def store(i, n):
        return pltpu.make_async_copy(
            held.at[i, n], pairs[i][1].at[pl.ds(n * each, each)], stored.at[i, n]
        )

    order = [(i, n) for n in range(chunks) for i in range(2)]
    for where in order:
        fetch(*where).start()
    for where in order:
        fetch(*where).wait()
        store(*where).start()
    for where in order:
        store(*where).wait()


def hand_over(first, second):
    chunks = 4
    dma = pltpu.SemaphoreType.DMA
    return pl.pallas_call(
        hand_over_kernel,
        out_shape=[jax.ShapeDtypeStruct(first.shape, F32)] * 2,
        in_specs=[pl.BlockSpec(memory_space=pltpu.HBM)] * 2,
        out_specs=[pl.BlockSpec(memory_space=pltpu.HBM)] * 2,
        scratch_shapes=[
            pltpu.VMEM((2, chunks, first.shape[0] // chunks) + first.shape[1:], F32),
            dma((2, chunks)), dma((2, chunks)),
        ],
        compiler_params=pltpu.CompilerParams(vmem_limit_bytes=67043328),
        name="hand_over",
    )(first, second)


def body(volts, cap, cond_x, cond_y, via, waveforms, placement, cells, wave_ids, amps):
    nx, ny = lax.axis_size("gx"), lax.axis_size("gy")
    devices = nx * ny
    size, layers, tile_x, tile_y = volts.shape
    steps = waveforms.shape[0] // size
    count = layers * tile_x
    capacity = 2 * cells.shape[0] // devices
    lane_count = min(capacity, 2 * LANES)
    halos = 1 + steps * ITERS
    packed = (2 * ITERS - 1) * size * size // LANES
    low_count = 2 * LANES
    high_count = tile_x * tile_y // low_count
    field = (layers, tile_x, size, LANES)
    dma = pltpu.SemaphoreType.DMA
    flat = (count, tile_y)
    many = (cells.shape[0] // LANES, LANES)
    out, residual = pl.pallas_call(
        functools.partial(grid_kernel, nx, ny, steps, layers, tile_x, capacity),
        out_shape=[jax.ShapeDtypeStruct((size, count, LANES), F32)] * 2,
        in_specs=[pl.BlockSpec(memory_space=pltpu.HBM)] * 10,
        out_specs=[pl.BlockSpec(memory_space=pltpu.HBM)] * 2,
        scratch_shapes=[
            pltpu.VMEM(field, F32),
            pltpu.VMEM(field, F32),
            *[pltpu.VMEM(flat, F32)] * 4,
            pltpu.VMEM(waveforms.shape, F32),
            *[pltpu.VMEM(many, jnp.int32)] * 3,
            pltpu.VMEM(many, F32),
            dma((9,)), dma((1,)), dma((2,)),
            pltpu.VMEM(field, F32),
            pltpu.VMEM(field, F32),
            pltpu.VMEM(field, F32),
            pltpu.VMEM(field, F32),
            pltpu.VMEM((2 * (ITERS + 1) * size, count * LANES), BF16),
            pltpu.VMEM((halos, 2, layers, size, LANES), BF16),
            pltpu.VMEM((halos, 2, layers, size, LANES), BF16),
            pltpu.VMEM((halos, size, LANES), F32),
            pltpu.VMEM((halos, 2, size, LANES), F32),
            pltpu.VMEM((steps, nx, packed, LANES), F32),
            pltpu.VMEM((steps, ny, packed, LANES), F32),
            pltpu.VMEM((steps, devices, size * size // LANES, LANES), F32),
            pltpu.VMEM((10,) + flat, F32),
            pltpu.VMEM((SUBLANES, LANES), F32),
            pltpu.VMEM(flat, F32),
            pltpu.VMEM(flat, F32),
            pltpu.VMEM(many, jnp.int32),
            pltpu.VMEM((4 * devices * capacity // lane_count, lane_count), F32),
            pltpu.VMEM((devices * SUBLANES, LANES), F32),
            pltpu.VMEM((devices, SUBLANES, LANES), F32),
            pltpu.VMEM((steps, 2 * size, waveforms.shape[1]), BF16),
            pltpu.VMEM((steps, high_count * size, low_count), F32),
            *[dma((2, 2))] * 4,
            *[dma((steps, ITERS - 1))] * 4,
            dma((2,)), dma((2,)), dma((1,)), dma((devices // 4,)),
            dma((steps,)), dma((steps,)),
        ],
        compiler_params=pltpu.CompilerParams(
            collective_id=0, has_side_effects=True, vmem_limit_bytes=67043328
        ),
        name="transient",
    )(
        volts.reshape(size, count, tile_y),
        *[x.reshape(flat) for x in (cap, cond_x, cond_y, via)],
        waveforms,
        *[x.reshape(many) for x in (placement, cells, wave_ids, amps)],
    )
    out, residual = hand_over(out, residual)
    return out.reshape(volts.shape), residual.reshape(volts.shape)


def solution(mesh):
    grid = P(None, "gx", "gy")
    field = P(None, None, "gx", "gy")
    flat = P(("gx", "gy"))
    return jax.shard_map(
        body,
        mesh=mesh,
        in_specs=(field, grid, grid, grid, grid, P(), P(("gx", "gy"), None), flat, flat, flat),
        out_specs=(field, field),
        check_vma=False,
    )
```
